8 devices in a mesh: dp: 1 (over z), tp: 2 (over y), sp: 4 (over x, core).
Axes of the slice: x: 2, y: 2, z: 1, core: 2. Of those that a mesh axis runs over, the one named last changes fastest.
Arguments:
- hidden: bfloat16 [96, 16384], P('dp')
- lengths: int32 [96], P('dp')
- k_cache: bfloat16 [96, 512, 8, 128], P('dp', 'sp', 'tp')
- v_cache: bfloat16 [96, 512, 8, 128], P('dp', 'sp', 'tp')
- norm_gain: bfloat16 [16384], replicated
- w_q: bfloat16 [16384, 16384], P(None, 'tp')
- w_k: bfloat16 [16384, 1024], P(None, 'tp')
- w_v: bfloat16 [16384, 1024], P(None, 'tp')
- w_o: bfloat16 [16384, 16384], P('tp')
- inv_freq: float32 [64], replicated
Outputs:
- output 1: bfloat16 [96, 16384], P('dp')
- output 2: bfloat16 [96, 512, 8, 128], P('dp', 'sp', 'tp')
- output 3: bfloat16 [96, 512, 8, 128], P('dp', 'sp', 'tp')
All inputs are finite; a program needn't handle non-finite values.
Results may differ from the reference program's by a relative error of at most 0.0088644.
Values sent between devices are 32-bit elements.
A program may use at most 2.5 GiB of HBM per device.

```python
import jax
import jax.numpy as jnp
from jax import lax

BATCH = 96
MODEL_DIM = 16384
NUM_HEADS = 128
KV_HEADS = 8
HEAD_DIM = 128
CACHE_LEN = 512

NORM_EPS = 1e-5
ROPE_BASE = 500000.0


def setup_inputs(seed: int = 0, part: int = 0) -> dict:
    part_key = jax.random.fold_in(jax.random.key(seed), part)
    key_list = jax.random.split(part_key, 5)
    len_keys = jax.random.split(jax.random.fold_in(part_key, 3), 4)
    shared = jax.random.split(jax.random.key(seed + 1), 6)
    hidden = 0.5 * jax.random.normal(key_list[0], (BATCH, MODEL_DIM), jnp.float32)
    long_len = jax.random.randint(len_keys[0], (BATCH,), 0, CACHE_LEN)
    short_len = jax.random.randint(len_keys[1], (BATCH,), 0, 8)
    pick_short = jax.random.randint(len_keys[2], (BATCH,), 0, 4) == 0
    perm_ids = jax.random.permutation(len_keys[3], BATCH)
    lengths = jnp.where(pick_short, short_len, long_len)
    lengths = lengths.at[perm_ids[0]].set(CACHE_LEN - 1).at[perm_ids[1]].set(0).astype(jnp.int32)
    k_cache = jax.random.normal(key_list[1], (BATCH, CACHE_LEN, KV_HEADS, HEAD_DIM), jnp.float32)
    seg_count = 64
    seg_ids = jnp.arange(CACHE_LEN) * seg_count // CACHE_LEN
    seg_means = jax.random.normal(key_list[2], (BATCH, seg_count, KV_HEADS, HEAD_DIM), jnp.float32)
    v_noise = jax.random.normal(key_list[3], (BATCH, CACHE_LEN, KV_HEADS, HEAD_DIM), jnp.float32)
    v_cache = 3.0 * seg_means[:, seg_ids] + v_noise
    norm_gain = 1.0 + 0.3 * jax.random.normal(shared[0], (MODEL_DIM,), jnp.float32)
    w_q = jax.random.normal(shared[1], (MODEL_DIM, NUM_HEADS * HEAD_DIM), jnp.float32) * MODEL_DIM ** -0.5
    w_k = jax.random.normal(shared[2], (MODEL_DIM, KV_HEADS * HEAD_DIM), jnp.float32) * MODEL_DIM ** -0.5
    w_v = jax.random.normal(shared[3], (MODEL_DIM, KV_HEADS * HEAD_DIM), jnp.float32) * MODEL_DIM ** -0.5
    w_o = jax.random.normal(shared[4], (NUM_HEADS * HEAD_DIM, MODEL_DIM), jnp.float32) * (NUM_HEADS * HEAD_DIM) ** -0.5
    exponent = jnp.arange(0, HEAD_DIM, 2).astype(jnp.float32) / HEAD_DIM
    jitter = jnp.exp(0.2 * jax.random.uniform(shared[5], (HEAD_DIM // 2,), jnp.float32, minval=-1.0, maxval=1.0))
    inv_freq = jnp.power(ROPE_BASE, -exponent) * jitter
    return {
        'hidden': hidden.astype(jnp.bfloat16),
        'lengths': lengths,
        'k_cache': k_cache.astype(jnp.bfloat16),
        'v_cache': v_cache.astype(jnp.bfloat16),
        'norm_gain': norm_gain.astype(jnp.bfloat16),
        'w_q': w_q.astype(jnp.bfloat16),
        'w_k': w_k.astype(jnp.bfloat16),
        'w_v': w_v.astype(jnp.bfloat16),
        'w_o': w_o.astype(jnp.bfloat16),
        'inv_freq': inv_freq.astype(jnp.float32),
    }


def rms_norm(hidden, norm_gain):
    hidden_f32 = hidden.astype(jnp.float32)
    inv_rms = lax.rsqrt(jnp.mean(hidden_f32 * hidden_f32, axis=-1, keepdims=True) + NORM_EPS)
    return (hidden_f32 * inv_rms * norm_gain.astype(jnp.float32)).astype(jnp.bfloat16)


def apply_rope(head_vec, angles):
    half_dim = head_vec.shape[-1] // 2
    vec_f32 = head_vec.astype(jnp.float32)
    cos_ang = jnp.cos(angles)[:, None, :]
    sin_ang = jnp.sin(angles)[:, None, :]
    lo_half = vec_f32[..., :half_dim]
    hi_half = vec_f32[..., half_dim:]
    rotated = jnp.concatenate([lo_half * cos_ang - hi_half * sin_ang, hi_half * cos_ang + lo_half * sin_ang], axis=-1)
    return rotated.astype(jnp.bfloat16)


def reference(hidden, lengths, k_cache, v_cache, norm_gain, w_q, w_k, w_v, w_o, inv_freq):
    normed = rms_norm(hidden, norm_gain)
    q_heads = jnp.dot(normed, w_q, preferred_element_type=jnp.float32).astype(jnp.bfloat16).reshape(BATCH, NUM_HEADS, HEAD_DIM)
    k_new = jnp.dot(normed, w_k, preferred_element_type=jnp.float32).astype(jnp.bfloat16).reshape(BATCH, KV_HEADS, HEAD_DIM)
    v_new = jnp.dot(normed, w_v, preferred_element_type=jnp.float32).astype(jnp.bfloat16).reshape(BATCH, KV_HEADS, HEAD_DIM)
    angles = lengths.astype(jnp.float32)[:, None] * inv_freq[None, :]
    q_rot = apply_rope(q_heads, angles)
    k_rot = apply_rope(k_new, angles)
    row_ids = jnp.arange(BATCH)
    k_out = k_cache.at[row_ids, lengths].set(k_rot)
    v_out = v_cache.at[row_ids, lengths].set(v_new)
    group_size = NUM_HEADS // KV_HEADS
    q_grp = q_rot.reshape(BATCH, KV_HEADS, group_size, HEAD_DIM)
    score_scale = HEAD_DIM ** -0.5

    def one_seq(seq_args):
        q_one, k_one, v_one, len_one = seq_args
        scores = jnp.einsum('kgd,skd->kgs', q_one.astype(jnp.float32), k_one.astype(jnp.float32)) * score_scale
        valid_mask = jnp.arange(CACHE_LEN) <= len_one
        scores = jnp.where(valid_mask, scores, -jnp.inf)
        top_score = jnp.max(scores, axis=-1, keepdims=True)
        weights = jnp.where(valid_mask, jnp.exp(scores - top_score), 0.0)
        weight_sum = jnp.sum(weights, axis=-1)
        weighted = jnp.einsum('kgs,skd->kgd', weights.astype(jnp.bfloat16).astype(jnp.float32), v_one.astype(jnp.float32))
        return (weighted / weight_sum[..., None]).astype(jnp.bfloat16)

    attn_out = lax.map(one_seq, (q_grp, k_out, v_out, lengths))
    attn_flat = attn_out.reshape(BATCH, NUM_HEADS * HEAD_DIM)
    proj_out = jnp.dot(attn_flat, w_o, preferred_element_type=jnp.float32)
    y_out = (hidden.astype(jnp.float32) + proj_out).astype(jnp.bfloat16)
    return (y_out, k_out, v_out)
```

```python
import functools

import jax
import jax.numpy as jnp
from jax import lax
from jax.experimental import pallas as pl
from jax.experimental.pallas import tpu as pltpu
from jax.sharding import PartitionSpec as P

NORM_EPS = 1e-5
HEAD = 128
KT = 2048
WIDE = 512
SLOTS = 12
MIB = 2 ** 20
MESH_ID = pl.DeviceIdType.MESH
SEQS = 8
RING = 8
AHEAD = 4
MASKED = -3e38
SCALE = HEAD ** -0.5
OUT_K = 4096
OUT_W = 512
OUT_SLOTS = 9
PIECE = 8


def rope(vec, cos_full, sin_signed):
    rounded = vec.astype(jnp.bfloat16).astype(jnp.float32)
    rotated = rounded * cos_full + pltpu.roll(rounded, 64, 1) * sin_signed
    return rotated.astype(jnp.bfloat16).astype(jnp.float32)


def qkv_kernel(len_ref, hid_hbm, gain_ref, freq_ref, wq, wk, wv, out_hbm,
               hid, normed, gain, trig, wbuf, acc, heads, hid_sem, w_sem, v_sem,
               x_send, x_recv, d_send, d_recv, f_send, f_recv, out_sem):
    batch, dim = hid.shape
    n_k = dim // KT
    n_head = heads.shape[1] - 2
    cols = n_head * HEAD
    n_wide = cols // WIDE - 1
    half = WIDE // 2
    t_wide = n_k
    t_tail = t_wide + n_wide * n_k
    t_end = t_tail + 2 * n_k
    s = lax.axis_index('sp')
    x_peer = lax.rem(s + 2, 4)
    d_peer = s + 1 - 2 * lax.rem(s, 2)

    units = [(0, 2)] + [(2 + 4 * u, 4) for u in range(n_wide)] + [(2 + 4 * n_wide, 2), (4 + 4 * n_wide, 2)]

    def slot_of(t):
        return lax.rem(t, SLOTS)

    def rows_of(k):
        return pl.ds(pl.multiple_of(k * KT, KT), KT)

    def kv_copies(t):
        lanes = pl.ds(pl.multiple_of(s * HEAD, HEAD), HEAD)
        slot = slot_of(t)
        return (pltpu.make_async_copy(wk.at[rows_of(t), lanes], wbuf.at[slot, :, pl.ds(0, HEAD)], w_sem.at[slot]),
                pltpu.make_async_copy(wv.at[rows_of(t), lanes], wbuf.at[slot, :, pl.ds(HEAD, HEAD)], v_sem.at[slot]))

    def wide_copy(t):
        i = t - t_wide
        lanes = pl.ds(pl.multiple_of(s * cols + lax.div(i, n_k) * WIDE, WIDE), WIDE)
        return pltpu.make_async_copy(wq.at[rows_of(lax.rem(i, n_k)), lanes], wbuf.at[slot_of(t)], w_sem.at[slot_of(t)])

    def tail_copy(t):
        i = t - t_tail
        lanes = pl.ds(pl.multiple_of(s * cols + n_wide * WIDE + lax.div(i, n_k) * half, half), half)
        return pltpu.make_async_copy(wq.at[rows_of(lax.rem(i, n_k)), lanes], wbuf.at[slot_of(t), :, pl.ds(0, half)], w_sem.at[slot_of(t)])

    def start_tile(t):
        @pl.when(t < t_tail)
        def _():
            wide_copy(t).start(priority=1)

        @pl.when((t >= t_tail) & (t < t_end))
        def _():
            tail_copy(t).start(priority=1)

    hid_copy = pltpu.make_async_copy(hid_hbm, hid, hid_sem)
    hid_copy.start()
    for t in range(n_k):
        for cp in kv_copies(t):
            cp.start(priority=1)
    for t in range(n_k, SLOTS):
        wide_copy(t).start(priority=1)

    barrier = pltpu.get_barrier_semaphore()
    for peer in (x_peer, d_peer):
        pl.semaphore_signal(barrier, inc=1, device_id={'sp': peer}, device_id_type=MESH_ID)
    pl.semaphore_wait(barrier, 2)

    freq = freq_ref[...]

    def angle_step(b, carry):
        trig[0, pl.ds(b, 1), :] = len_ref[b].astype(jnp.float32) * freq
        return carry

    lax.fori_loop(0, batch, angle_step, 0)
    angles = trig[0]
    sin_full = jnp.sin(angles)
    lane = lax.broadcasted_iota(jnp.int32, sin_full.shape, 1)
    trig[1] = jnp.where(lane < 64, -sin_full, sin_full)
    trig[0] = jnp.cos(angles)
    gain[...] = gain_ref[...].astype(jnp.float32)

    hid_copy.wait()
    step = 512

    def sq_step(i, acc):
        x = hid[:, pl.ds(pl.multiple_of(i * step, step), step)].astype(jnp.float32)
        x = x * x
        for t in range(step // 128):
            acc = acc + x[:, t * 128:(t + 1) * 128]
        return acc

    sq = lax.fori_loop(0, dim // step, sq_step, jnp.zeros((batch, 128), jnp.float32))
    inv = lax.rsqrt(jnp.sum(sq, axis=1, keepdims=True) / dim + NORM_EPS)
    inv = jnp.broadcast_to(inv, (batch, 128))

    def norm_step(i, carry):
        for t in range(step // 128):
            sl = pl.ds(pl.multiple_of(i * step + t * 128, 128), 128)
            x = hid[:, sl].astype(jnp.float32)
            row = gain[pl.ds(i * (step // 128) + t, 1), :]
            normed[:, sl] = (x * inv * row).astype(jnp.bfloat16)
        return carry

    lax.fori_loop(0, dim // step, norm_step, 0)

    def copy_of(kind, group, u, start, size):
        send_sem, recv_sem, peer = {'x': (x_send, x_recv, x_peer), 'd': (d_send, d_recv, d_peer), 'f': (f_send, f_recv, d_peer)}[kind]
        part = heads.at[group, pl.ds(start, size)]
        return pltpu.make_async_remote_copy(part, part, send_sem.at[u], recv_sem.at[u], device_id={'sp': peer}, device_id_type=MESH_ID)

    def publish(u, start, size):
        copy_of('x', s, u, start, size).start()
        copy_of('d', s, u, start, size).start()

    def forward(u):
        copy_of('x', x_peer, u, *units[u]).wait_recv()
        copy_of('f', x_peer, u, *units[u]).start()

    def multiply(t, k, width):
        part = jnp.dot(normed[:, rows_of(k)], wbuf[slot_of(t), :, pl.ds(0, width)], preferred_element_type=jnp.float32)

        @pl.when(k == 0)
        def _():
            acc[:, pl.ds(0, width)] = part

        @pl.when(k > 0)
        def _():
            acc[:, pl.ds(0, width)] += part

    def kv_step(t, carry):
        for cp in kv_copies(t):
            cp.wait()
        multiply(t, t, half)
        start_tile(t + SLOTS)
        return carry

    lax.fori_loop(0, n_k, kv_step, 0)
    heads[s, 0] = rope(acc[:, :HEAD], trig[0], trig[1])
    heads[s, 1] = acc[:, HEAD:2 * HEAD].astype(jnp.bfloat16).astype(jnp.float32)
    publish(0, *units[0])

    def wide_step(i, carry):
        t = i + t_wide
        k = lax.rem(i, n_k)
        chunk = lax.div(i, n_k)
        wide_copy(t).wait()
        multiply(t, k, WIDE)
        start_tile(t + SLOTS)

        @pl.when(k == n_k - 1)
        def _():
            first = 2 + 4 * chunk
            for h in range(4):
                heads[s, first + h] = rope(acc[:, h * HEAD:(h + 1) * HEAD], trig[0], trig[1])
            publish(chunk + 1, first, 4)

        for u in range(n_wide - 1):
            @pl.when(i == (u + 1) * n_k + 3)
            def _():
                forward(u)
        return carry

    lax.fori_loop(0, n_wide * n_k, wide_step, 0)

    def tail_step(i, carry):
        t = i + t_tail
        k = lax.rem(i, n_k)
        chunk = lax.div(i, n_k)
        tail_copy(t).wait()
        multiply(t, k, half)
        start_tile(t + SLOTS)

        @pl.when(k == n_k - 1)
        def _():
            first = 2 + 4 * n_wide + 2 * chunk
            for h in range(2):
                heads[s, first + h] = rope(acc[:, h * HEAD:(h + 1) * HEAD], trig[0], trig[1])
            publish(chunk + n_wide + 1, first, 2)

        for c in range(2):
            @pl.when(i == c * n_k + 4)
            def _():
                forward(n_wide - 1 + c)
        return carry

    lax.fori_loop(0, 2 * n_k, tail_step, 0)
    forward(n_wide + 1)
    forward(n_wide + 2)
    f_peer = lax.rem(d_peer + 2, 4)
    outs = [pltpu.make_async_copy(heads.at[g], out_hbm.at[g], out_sem.at[i]) for i, g in enumerate((s, x_peer, d_peer, f_peer))]
    outs[0].start()
    outs[1].start()
    for u, unit in enumerate(units):
        copy_of('d', d_peer, u, *unit).wait_recv()
    outs[2].start()
    for u, unit in enumerate(units):
        copy_of('f', f_peer, u, *unit).wait_recv()
    outs[3].start()
    for u, unit in enumerate(units):
        copy_of('x', s, u, *unit).wait_send()
        copy_of('d', s, u, *unit).wait_send()
        copy_of('f', x_peer, u, *unit).wait_send()
    for cp in outs:
        cp.wait()


def project(hidden, lengths, norm_gain, w_q, w_k, w_v, inv_freq):
    batch, dim = hidden.shape
    sp = 4
    n_head = w_q.shape[1] // sp // HEAD
    n_unit = n_head * HEAD // WIDE + 2
    freq = jnp.concatenate([inv_freq, inv_freq]).reshape(1, HEAD)
    vmem = pl.BlockSpec(memory_space=pltpu.VMEM)
    hbm = pl.BlockSpec(memory_space=pl.ANY)
    dma = pltpu.SemaphoreType.DMA
    return pl.pallas_call(
        qkv_kernel,
        out_shape=jax.ShapeDtypeStruct((sp, 2 + n_head, batch, HEAD), jnp.float32),
        in_specs=[pl.BlockSpec(memory_space=pltpu.SMEM), hbm, vmem, vmem, hbm, hbm, hbm],
        out_specs=hbm,
        scratch_shapes=[
            pltpu.VMEM((batch, dim), jnp.bfloat16),
            pltpu.VMEM((batch, dim), jnp.bfloat16),
            pltpu.VMEM((dim // HEAD, HEAD), jnp.float32),
            pltpu.VMEM((2, batch, HEAD), jnp.float32),
            pltpu.VMEM((SLOTS, KT, WIDE), jnp.bfloat16),
            pltpu.VMEM((batch, WIDE), jnp.float32),
            pltpu.VMEM((sp, 2 + n_head, batch, HEAD), jnp.float32),
            dma, dma((SLOTS,)), dma((SLOTS,)),
            dma((n_unit,)), dma((n_unit,)), dma((n_unit,)), dma((n_unit,)), dma((n_unit,)), dma((n_unit,)),
            dma((4,)),
        ],
        compiler_params=pltpu.CompilerParams(collective_id=0, has_side_effects=True, vmem_limit_bytes=60 * MIB),
        cost_estimate=pl.CostEstimate(flops=2 * batch * dim * (n_head + 2) * HEAD, bytes_accessed=2 * dim * (n_head + 2) * HEAD, transcendentals=0),
        name='qkv_exchange',
    )(lengths, hidden, norm_gain.reshape(dim // HEAD, HEAD), freq, w_q, w_k, w_v)


def attend_kernel(len_ref, k_hbm, v_hbm, qkv, k_out, v_out, o_ref, ml_ref,
                  kbuf, vbuf, slot_of, ml_rows, k_sem, v_sem, ko_sem, vo_sem):
    batch, rows, _ = k_hbm.shape
    n_kv = 4
    slots = rows // n_kv
    n_chunk = batch // SEQS
    n_unit = qkv.shape[0] // (n_kv * batch)
    group = n_unit - 2
    n_head = n_kv * group
    start = lax.axis_index('sp') * slots

    def in_copies(i):
        r = lax.rem(i, RING)
        seqs = pl.ds(i * SEQS, SEQS)
        return (pltpu.make_async_copy(k_hbm.at[seqs], kbuf.at[r], k_sem.at[r]),
                pltpu.make_async_copy(v_hbm.at[seqs], vbuf.at[r], v_sem.at[r]))

    def out_copies(i):
        r = lax.rem(i, RING)
        seqs = pl.ds(i * SEQS, SEQS)
        return (pltpu.make_async_copy(kbuf.at[r], k_out.at[seqs], ko_sem.at[r]),
                pltpu.make_async_copy(vbuf.at[r], v_out.at[seqs], vo_sem.at[r]))

    for i in range(AHEAD):
        for cp in in_copies(i):
            cp.start()

    row = lax.broadcasted_iota(jnp.int32, (n_head, rows), 0)
    col = lax.broadcasted_iota(jnp.int32, (n_head, rows), 1)
    slot_of[...] = jnp.where(lax.rem(col, n_kv) == lax.div(row, group), lax.div(col, n_kv), 2 ** 30)
    win_row = lax.broadcasted_iota(jnp.int32, (16, HEAD), 0)
    lane = lax.broadcasted_iota(jnp.int32, (n_head, HEAD), 1)

    def new_rows(offset, b):
        four = qkv[pl.ds(offset * batch + b, n_kv, stride=n_unit * batch), :]
        return jnp.concatenate([four] * 4, axis=0).astype(jnp.bfloat16)

    def chunk_step(i, carry):
        r = lax.rem(i, RING)

        @pl.when(i + AHEAD < n_chunk)
        def _():
            @pl.when(i + AHEAD >= RING)
            def _():
                for cp in out_copies(i + AHEAD - RING):
                    cp.wait()
            for cp in in_copies(i + AHEAD):
                cp.start()

        for cp in in_copies(i):
            cp.wait()
        for j in range(SEQS):
            b = i * SEQS + j
            pos = len_ref[b] - start
            held = jnp.clip(pos, 0, slots - 1)
            window = pl.ds(pl.multiple_of(lax.div(held, 4) * 16, 16), 16)
            pick = lax.div(win_row, n_kv) == jnp.where(held == pos, lax.rem(held, 4), -1)
            kbuf[r, j, window, :] = jnp.where(pick, new_rows(0, b), kbuf[r, j, window, :])
            vbuf[r, j, window, :] = jnp.where(pick, new_rows(1, b), vbuf[r, j, window, :])
        for cp in out_copies(i):
            cp.start()
        def scores_of(j):
            b = i * SEQS + j
            q = jnp.concatenate([qkv[pl.ds((g * n_unit + 2) * batch + b, group, stride=batch), :] for g in range(n_kv)], axis=0)
            return lax.dot_general(q.astype(jnp.bfloat16), kbuf[r, j], (((1,), (1,)), ((), ())), preferred_element_type=jnp.float32)

        def softmax_of(j, scores):
            valid = slot_of[...] <= len_ref[i * SEQS + j] - start
            scores = jnp.where(valid, scores, MASKED)
            top = jnp.max(scores, axis=1, keepdims=True)
            weights = jnp.where(valid, jnp.exp((scores - top) * SCALE), 0.0)
            return weights.astype(jnp.bfloat16), top, jnp.sum(weights, axis=1, keepdims=True)

        def finish(j, weights, top, total):
            b = i * SEQS + j
            o_ref[pl.ds(b, n_head, stride=batch), :] = jnp.dot(weights, vbuf[r, j], preferred_element_type=jnp.float32)
            ml_rows[pl.ds(b, n_head, stride=batch), :] = jnp.where(lane < n_head, top * SCALE, total)

        sc = [scores_of(j) for j in range(SEQS)]
        sm = [softmax_of(j, sc[j]) for j in range(SEQS)]
        for j in range(SEQS):
            finish(j, *sm[j])
        return carry

    lax.fori_loop(0, n_chunk, chunk_step, 0)
    out_lane = lax.broadcasted_iota(jnp.int32, (batch, HEAD), 1)

    def gather_step(h, acc):
        mine = lax.rem(out_lane, n_head) == h
        return jnp.where(mine, ml_rows[pl.ds(pl.multiple_of(h * batch, 8), batch), :], acc)

    ml_ref[...] = lax.fori_loop(0, n_head, gather_step, jnp.zeros((batch, HEAD), jnp.float32))

    def drain(i, carry):
        for cp in out_copies(i):
            cp.wait()
        return carry

    lax.fori_loop(n_chunk - RING, n_chunk, drain, 0)


def attend(qkv, lengths, k_cache, v_cache):
    batch, slots, n_kv, head = k_cache.shape
    rows = slots * n_kv
    n_head = n_kv * (qkv.shape[1] - 2)
    flat = (batch, rows, head)
    smem = pl.BlockSpec(memory_space=pltpu.SMEM)
    vmem = pl.BlockSpec(memory_space=pltpu.VMEM)
    hbm = pl.BlockSpec(memory_space=pl.ANY)
    dma = pltpu.SemaphoreType.DMA((RING,))
    k_new, v_new, out, ml = pl.pallas_call(
        attend_kernel,
        out_shape=(jax.ShapeDtypeStruct(flat, jnp.bfloat16), jax.ShapeDtypeStruct(flat, jnp.bfloat16),
                   jax.ShapeDtypeStruct((n_head * batch, head), jnp.float32), jax.ShapeDtypeStruct((batch, head), jnp.float32)),
        in_specs=[smem, hbm, hbm, vmem],
        out_specs=(hbm, hbm, vmem, vmem),
        scratch_shapes=[
            pltpu.VMEM((RING, SEQS, rows, head), jnp.bfloat16),
            pltpu.VMEM((RING, SEQS, rows, head), jnp.bfloat16),
            pltpu.VMEM((n_head, rows), jnp.int32),
            pltpu.VMEM((n_head * batch, head), jnp.float32),
            dma, dma, dma, dma,
        ],
        compiler_params=pltpu.CompilerParams(vmem_limit_bytes=50 * MIB),
        cost_estimate=pl.CostEstimate(flops=4 * batch * n_head * rows * head, bytes_accessed=8 * batch * rows * head, transcendentals=0),
        name='attend_local',
    )(lengths, k_cache.reshape(flat), v_cache.reshape(flat), qkv.reshape(-1, head))
    return k_new.reshape(k_cache.shape), v_new.reshape(v_cache.shape), out, ml


def combine_kernel(o_hbm, ml_ref, hid_hbm, wo, y_hbm,
                   own, other, ml_all, gates, mine, x_out, x_in, d_out, d_in, obf, hid, wbuf,
                   part, part_in, fin, fin_x, fin_d, fin_f, ybf,
                   own_sem, hid_sem, w_sem, y_sem, ml_send, ml_recv, o_send, o_recv, x_send, x_recv, d_send, d_recv,
                   p_send, p_recv, fx_send, fx_recv, fd_send, fd_recv, ff_send, ff_recv):
    n_head, batch, _ = o_hbm.shape
    rows = batch // 2
    half = n_head // 2
    n_piece = half // PIECE
    n_k = wo.shape[0] // OUT_K
    cols = wo.shape[1] // 2
    n_col = cols // OUT_W
    n_tile = n_col * n_k
    tp = lax.axis_index('tp')
    s = lax.axis_index('sp')
    x = lax.div(s, 2)
    c = lax.rem(s, 2)
    x_peer = lax.rem(s + 2, 4)
    d_peer = s + 1 - 2 * c
    diag = 3 - s
    my_rows = pl.ds(pl.multiple_of(x * rows, 16), rows)
    peer_rows = pl.ds(pl.multiple_of((1 - x) * rows, 16), rows)

    def remote(src, dst, send_sem, recv_sem, peer):
        device = {'sp': peer} if peer is not None else {'tp': 1 - tp}
        return pltpu.make_async_remote_copy(src, dst, send_sem, recv_sem, device_id=device, device_id_type=MESH_ID)

    def w_copy(t):
        lanes = pl.ds(pl.multiple_of(c * cols + lax.div(t, n_k) * OUT_W, OUT_W), OUT_W)
        depth = pl.ds(pl.multiple_of(lax.rem(t, n_k) * OUT_K, OUT_K), OUT_K)
        slot = lax.rem(t, OUT_SLOTS)
        return pltpu.make_async_copy(wo.at[depth, lanes], wbuf.at[slot], w_sem.at[slot])

    own_copy = pltpu.make_async_copy(o_hbm.at[pl.ds(c * half, half)], own, own_sem)
    own_copy.start()
    hid_copy = pltpu.make_async_copy(hid_hbm.at[my_rows, pl.ds(pl.multiple_of(c * cols, cols), cols)], hid, hid_sem)
    hid_copy.start()
    for t in range(OUT_SLOTS):
        w_copy(t).start(priority=1)

    barrier = pltpu.get_barrier_semaphore()
    for device in ({'sp': x_peer}, {'sp': d_peer}, {'sp': diag}, {'tp': 1 - tp}):
        pl.semaphore_signal(barrier, inc=1, device_id=device, device_id_type=MESH_ID)
    pl.semaphore_wait(barrier, 4)

    ml_copies = [remote(ml_ref, ml_all.at[i], ml_send.at[i], ml_recv.at[i], peer) for i, peer in enumerate((x_peer, d_peer, diag))]
    for cp in ml_copies:
        cp.start()

    def o_copy(p):
        return remote(o_hbm.at[pl.ds((1 - c) * half + p * PIECE, PIECE)], other.at[pl.ds(p * PIECE, PIECE)], o_send.at[p], o_recv.at[p], d_peer)

    for p in range(n_piece):
        o_copy(p).start()

    for cp in ml_copies:
        cp.wait()
    stats = [ml_ref[...], ml_all[1], ml_all[0], ml_all[2]]
    top = functools.reduce(jnp.maximum, stats)
    factors = [jnp.exp(m - top) for m in stats]
    total = functools.reduce(jnp.add, [f * pltpu.roll(m, n_head, 1) for f, m in zip(factors, stats)])
    for i in range(2):
        gate = factors[i] / total
        gates[i] = jnp.where(c == 0, gate, pltpu.roll(gate, HEAD - half, 1))
    own_copy.wait()

    def x_copy(p):
        part_of = pl.ds(p * PIECE, PIECE)
        return remote(x_out.at[part_of], x_in.at[part_of], x_send.at[p], x_recv.at[p], x_peer)

    def weigh(p, which):
        mine_gate = gates[0, which, :]
        other_gate = gates[1, which, :]
        out = []
        for h in range(PIECE):
            i = p * PIECE + h
            out.append(mine_gate[:, h:h + 1] * own[i, which, :] + other_gate[:, h:h + 1] * other[i, which, :])
        return out

    def mix_step(p, carry):
        o_copy(p).wait_recv()
        for h, val in enumerate(weigh(p, peer_rows)):
            x_out[p * PIECE + h] = val
        x_copy(p).start()
        for h, val in enumerate(weigh(p, my_rows)):
            mine[p * PIECE + h] = val
        gates[0] = pltpu.roll(gates[0], HEAD - PIECE, 1)
        gates[1] = pltpu.roll(gates[1], HEAD - PIECE, 1)
        return carry

    lax.fori_loop(0, n_piece, mix_step, 0)

    def d_copy(p):
        part_of = pl.ds(p * PIECE, PIECE)
        return remote(d_out.at[part_of], d_in.at[part_of], d_send.at[p], d_recv.at[p], d_peer)

    def head_lanes(h):
        return pl.ds(pl.multiple_of(h * HEAD, HEAD), HEAD)

    def merge_step(p, carry):
        x_copy(p).wait_recv()
        for h in range(PIECE):
            i = p * PIECE + h
            val = (mine[i] + x_in[i]).astype(jnp.bfloat16)
            obf[:, head_lanes(c * half + i)] = val
            d_out[i] = val.astype(jnp.float32)
        d_copy(p).start()
        return carry

    lax.fori_loop(0, n_piece, merge_step, 0)

    def spread_step(p, carry):
        d_copy(p).wait_recv()
        for h in range(PIECE):
            i = p * PIECE + h
            obf[:, head_lanes((1 - c) * half + i)] = d_in[i].astype(jnp.bfloat16)
        return carry

    lax.fori_loop(0, n_piece, spread_step, 0)
    hid_copy.wait()

    def p_copy(j):
        return remote(part.at[j], part_in.at[j], p_send.at[j], p_recv.at[j], None)

    def fx_copy(j):
        return remote(fin.at[j], fin_x.at[j], fx_send.at[j], fx_recv.at[j], x_peer)

    def fd_copy(j):
        return remote(fin.at[j], fin_d.at[j], fd_send.at[j], fd_recv.at[j], d_peer)

    def ff_copy(j):
        return remote(fin_x.at[j], fin_f.at[j], ff_send.at[j], ff_recv.at[j], d_peer)

    def lanes_of(j, core):
        return pl.ds(pl.multiple_of(core * cols + j * OUT_W, OUT_W), OUT_W)

    def y_copies(j):
        return [pltpu.make_async_copy(ybf.at[:, lanes_of(j, core)], y_hbm.at[:, lanes_of(j, core)], y_sem.at[core, j]) for core in range(2)]

    def finish(j):
        p_copy(j).wait_recv()
        lane = pl.ds(pl.multiple_of(j * OUT_W, OUT_W), OUT_W)
        val = (hid[:, lane].astype(jnp.float32) + (part[j] + part_in[j])).astype(jnp.bfloat16)
        ybf[my_rows, lanes_of(j, c)] = val
        fin[j] = val.astype(jnp.float32)
        fx_copy(j).start()
        fd_copy(j).start()

    def pass_on(j):
        fx_copy(j).wait_recv()
        ff_copy(j).start()
        ybf[peer_rows, lanes_of(j, c)] = fin_x[j].astype(jnp.bfloat16)
        fd_copy(j).wait_recv()
        ybf[my_rows, lanes_of(j, 1 - c)] = fin_d[j].astype(jnp.bfloat16)

    def deliver(j):
        ff_copy(j).wait_recv()
        ybf[peer_rows, lanes_of(j, 1 - c)] = fin_f[j].astype(jnp.bfloat16)
        for cp in y_copies(j):
            cp.start()

    lags = (2, 4, 5)

    def col_step(j, carry):
        @pl.when(j < n_col)
        def _():
            acc = None
            for k in range(n_k):
                t = j * n_k + k
                w_copy(t).wait()
                term = jnp.dot(obf[:, k * OUT_K:(k + 1) * OUT_K], wbuf[lax.rem(t, OUT_SLOTS)], preferred_element_type=jnp.float32)
                acc = term if acc is None else acc + term

                @pl.when(t + OUT_SLOTS < n_tile)
                def _():
                    w_copy(t + OUT_SLOTS).start(priority=1)
            part[j] = acc
            p_copy(j).start()

        for lag, stage in zip(lags, (finish, pass_on, deliver)):
            @pl.when((j >= lag) & (j - lag < n_col))
            def _():
                stage(j - lag)
        return carry

    lax.fori_loop(0, n_col + lags[-1], col_step, 0)

    for p in range(n_piece):
        o_copy(p).wait_send()
        x_copy(p).wait_send()
        d_copy(p).wait_send()

    def drain(j, carry):
        p_copy(j).wait_send()
        fx_copy(j).wait_send()
        fd_copy(j).wait_send()
        ff_copy(j).wait_send()
        for cp in y_copies(j):
            cp.wait()
        return carry

    lax.fori_loop(0, n_col, drain, 0)


def combine(out, ml, hidden, w_o):
    batch, dim = hidden.shape
    n_head = out.shape[0] // batch
    rows = batch // 2
    half = n_head // 2
    n_piece = half // PIECE
    n_col = dim // 2 // OUT_W
    vmem = pl.BlockSpec(memory_space=pltpu.VMEM)
    hbm = pl.BlockSpec(memory_space=pl.ANY)
    dma = pltpu.SemaphoreType.DMA
    f32 = jnp.float32
    quad = pltpu.VMEM((half, rows, HEAD), f32)
    tiles = pltpu.VMEM((n_col, rows, OUT_W), f32)
    return pl.pallas_call(
        combine_kernel,
        out_shape=jax.ShapeDtypeStruct((batch, dim), jnp.bfloat16),
        in_specs=[hbm, vmem, hbm, hbm],
        out_specs=hbm,
        scratch_shapes=[
            pltpu.VMEM((half, batch, HEAD), f32), pltpu.VMEM((half, batch, HEAD), f32),
            pltpu.VMEM((3, batch, HEAD), f32), pltpu.VMEM((2, batch, HEAD), f32),
            quad, quad, quad, quad, quad,
            pltpu.VMEM((rows, n_head * HEAD), jnp.bfloat16), pltpu.VMEM((rows, dim // 2), jnp.bfloat16),
            pltpu.VMEM((OUT_SLOTS, OUT_K, OUT_W), jnp.bfloat16),
            tiles, tiles, tiles, tiles, tiles, tiles,
            pltpu.VMEM((batch, dim), jnp.bfloat16),
            dma, dma, dma((OUT_SLOTS,)), dma((2, n_col)), dma((3,)), dma((3,)),
            dma((n_piece,)), dma((n_piece,)), dma((n_piece,)), dma((n_piece,)), dma((n_piece,)), dma((n_piece,)),
            dma((n_col,)), dma((n_col,)), dma((n_col,)), dma((n_col,)), dma((n_col,)), dma((n_col,)), dma((n_col,)), dma((n_col,)),
        ],
        compiler_params=pltpu.CompilerParams(collective_id=1, has_side_effects=True, vmem_limit_bytes=63 * MIB),
        cost_estimate=pl.CostEstimate(flops=batch * dim * n_head * HEAD, bytes_accessed=dim * n_head * HEAD, transcendentals=0),
        name='combine_project',
    )(out.reshape(n_head, batch, HEAD), ml, hidden, w_o)


def device_step(hidden, lengths, k_cache, v_cache, norm_gain, w_q, w_k, w_v, w_o, inv_freq):
    qkv = project(hidden, lengths, norm_gain, w_q, w_k, w_v, inv_freq)
    k_new, v_new, out, ml = attend(qkv, lengths, k_cache, v_cache)
    return combine(out, ml, hidden, w_o), k_new, v_new


def solution(mesh):
    cache_spec = P('dp', 'sp', 'tp', None)
    in_specs = (P('dp', None), P('dp'), cache_spec, cache_spec, P(None), P(None, 'tp'), P(None, 'tp'), P(None, 'tp'), P('tp', None), P(None))
    out_specs = (P('dp', None), cache_spec, cache_spec)
    return jax.shard_map(device_step, mesh=mesh, in_specs=in_specs, out_specs=out_specs, check_vma=False)
```

```python
import functools

import jax
import jax.numpy as jnp
from jax import lax
from jax.experimental import pallas as pl
from jax.experimental.pallas import tpu as pltpu
from jax.sharding import PartitionSpec as P

NORM_EPS = 1e-5
HEAD = 128
KT = 2048
WIDE = 512
SLOTS = 16
MIB = 2 ** 20
MESH_ID = pl.DeviceIdType.MESH
SEQS = 8
RING = 8
AHEAD = 4
MASKED = -3e38
SCALE = HEAD ** -0.5
OUT_K = 8192
OUT_W = 256
OUT_SLOTS = 6
PIECE = 8


def rope(vec, cos_full, sin_signed):
    rounded = vec.astype(jnp.bfloat16).astype(jnp.float32)
    rotated = rounded * cos_full + pltpu.roll(rounded, 64, 1) * sin_signed
    return rotated.astype(jnp.bfloat16).astype(jnp.float32)


def qkv_kernel(len_ref, hid_hbm, gain_ref, freq_ref, wq, wk, wv, out_hbm,
               hid, normed, gain, trig, wbuf, acc, heads, hid_sem, w_sem, v_sem,
               x_send, x_recv, d_send, d_recv, f_send, f_recv, out_sem):
    batch, dim = hid.shape
    n_k = dim // KT
    n_head = heads.shape[1] - 2
    cols = n_head * HEAD
    n_wide = cols // WIDE - 1
    half = WIDE // 2
    t_wide = n_k
    t_tail = t_wide + n_wide * n_k
    t_end = t_tail + 2 * n_k
    s = lax.axis_index('sp')
    x_peer = lax.rem(s + 2, 4)
    d_peer = s + 1 - 2 * lax.rem(s, 2)

    units = [(0, 2)] + [(2 + 4 * u, 4) for u in range(n_wide)] + [(2 + 4 * n_wide, 2), (4 + 4 * n_wide, 2)]

    def slot_of(t):
        return lax.rem(t, SLOTS)

    def rows_of(k):
        return pl.ds(pl.multiple_of(k * KT, KT), KT)

    def kv_copies(t):
        lanes = pl.ds(pl.multiple_of(s * HEAD, HEAD), HEAD)
        slot = slot_of(t)
        return (pltpu.make_async_copy(wk.at[rows_of(t), lanes], wbuf.at[slot, :, pl.ds(0, HEAD)], w_sem.at[slot]),
                pltpu.make_async_copy(wv.at[rows_of(t), lanes], wbuf.at[slot, :, pl.ds(HEAD, HEAD)], v_sem.at[slot]))

    def wide_copy(t):
        i = t - t_wide
        lanes = pl.ds(pl.multiple_of(s * cols + lax.div(i, n_k) * WIDE, WIDE), WIDE)
        return pltpu.make_async_copy(wq.at[rows_of(lax.rem(i, n_k)), lanes], wbuf.at[slot_of(t)], w_sem.at[slot_of(t)])

    def tail_copy(t):
        i = t - t_tail
        lanes = pl.ds(pl.multiple_of(s * cols + n_wide * WIDE + lax.div(i, n_k) * half, half), half)
        return pltpu.make_async_copy(wq.at[rows_of(lax.rem(i, n_k)), lanes], wbuf.at[slot_of(t), :, pl.ds(0, half)], w_sem.at[slot_of(t)])

    def start_tile(t):
        @pl.when(t < t_tail)
        def _():
            wide_copy(t).start(priority=1)

        @pl.when((t >= t_tail) & (t < t_end))
        def _():
            tail_copy(t).start(priority=1)

    hid_copy = pltpu.make_async_copy(hid_hbm, hid, hid_sem)
    hid_copy.start()
    for t in range(n_k):
        for cp in kv_copies(t):
            cp.start(priority=1)
    for t in range(n_k, SLOTS):
        wide_copy(t).start(priority=1)

    barrier = pltpu.get_barrier_semaphore()
    for peer in (x_peer, d_peer):
        pl.semaphore_signal(barrier, inc=1, device_id={'sp': peer}, device_id_type=MESH_ID)

    freq = jnp.concatenate([freq_ref[...], freq_ref[...]], axis=1)

    def angle_step(b, carry):
        trig[0, pl.ds(b, 1), :] = len_ref[b].astype(jnp.float32) * freq
        return carry

    lax.fori_loop(0, batch, angle_step, 0)
    angles = trig[0]
    sin_full = jnp.sin(angles)
    lane = lax.broadcasted_iota(jnp.int32, sin_full.shape, 1)
    trig[1] = jnp.where(lane < 64, -sin_full, sin_full)
    trig[0] = jnp.cos(angles)
    gain[...] = gain_ref[...].astype(jnp.float32)

    hid_copy.wait()
    step = 512

    def sq_step(i, acc):
        x = hid[:, pl.ds(pl.multiple_of(i * step, step), step)].astype(jnp.float32)
        x = x * x
        for t in range(step // 128):
            acc = acc + x[:, t * 128:(t + 1) * 128]
        return acc

    sq = lax.fori_loop(0, dim // step, sq_step, jnp.zeros((batch, 128), jnp.float32))
    inv = lax.rsqrt(jnp.sum(sq, axis=1, keepdims=True) / dim + NORM_EPS)
    inv = jnp.broadcast_to(inv, (batch, 128))

    def norm_step(i, carry):
        for t in range(step // 128):
            sl = pl.ds(pl.multiple_of(i * step + t * 128, 128), 128)
            x = hid[:, sl].astype(jnp.float32)
            row = gain[pl.ds(i * (step // 128) + t, 1), :]
            normed[:, sl] = (x * inv * row).astype(jnp.bfloat16)
        return carry

    lax.fori_loop(0, dim // step, norm_step, 0)

    def copy_of(kind, group, u, start, size):
        send_sem, recv_sem, peer = {'x': (x_send, x_recv, x_peer), 'd': (d_send, d_recv, d_peer), 'f': (f_send, f_recv, d_peer)}[kind]
        part = heads.at[group, pl.ds(start, size)]
        return pltpu.make_async_remote_copy(part, part, send_sem.at[u], recv_sem.at[u], device_id={'sp': peer}, device_id_type=MESH_ID)

    def publish(u, start, size):
        copy_of('x', s, u, start, size).start()
        copy_of('d', s, u, start, size).start()

    def forward(u):
        copy_of('x', x_peer, u, *units[u]).wait_recv()
        copy_of('f', x_peer, u, *units[u]).start()

    def multiply(t, k, width):
        part = jnp.dot(normed[:, rows_of(k)], wbuf[slot_of(t), :, pl.ds(0, width)], preferred_element_type=jnp.float32)

        @pl.when(k == 0)
        def _():
            acc[:, pl.ds(0, width)] = part

        @pl.when(k > 0)
        def _():
            acc[:, pl.ds(0, width)] += part

    def kv_step(t, carry):
        for cp in kv_copies(t):
            cp.wait()
        multiply(t, t, half)
        start_tile(t + SLOTS)
        return carry

    lax.fori_loop(0, n_k, kv_step, 0)
    pl.semaphore_wait(barrier, 2)
    heads[s, 0] = rope(acc[:, :HEAD], trig[0], trig[1])
    heads[s, 1] = acc[:, HEAD:2 * HEAD].astype(jnp.bfloat16).astype(jnp.float32)
    publish(0, *units[0])

    def wide_step(i, carry):
        t = i + t_wide
        k = lax.rem(i, n_k)
        chunk = lax.div(i, n_k)
        wide_copy(t).wait()
        multiply(t, k, WIDE)
        start_tile(t + SLOTS)

        @pl.when(k == n_k - 1)
        def _():
            first = 2 + 4 * chunk
            for h in range(4):
                heads[s, first + h] = rope(acc[:, h * HEAD:(h + 1) * HEAD], trig[0], trig[1])
            publish(chunk + 1, first, 4)

        for u in range(n_wide - 1):
            @pl.when(i == (u + 1) * n_k + 3)
            def _():
                forward(u)
        return carry

    lax.fori_loop(0, n_wide * n_k, wide_step, 0)

    def tail_step(i, carry):
        t = i + t_tail
        k = lax.rem(i, n_k)
        chunk = lax.div(i, n_k)
        tail_copy(t).wait()
        multiply(t, k, half)
        start_tile(t + SLOTS)

        @pl.when(k == n_k - 1)
        def _():
            first = 2 + 4 * n_wide + 2 * chunk
            for h in range(2):
                heads[s, first + h] = rope(acc[:, h * HEAD:(h + 1) * HEAD], trig[0], trig[1])
            publish(chunk + n_wide + 1, first, 2)

        for c in range(2):
            @pl.when(i == c * n_k + 4)
            def _():
                forward(n_wide - 1 + c)
        return carry

    lax.fori_loop(0, 2 * n_k, tail_step, 0)
    forward(n_wide + 1)
    forward(n_wide + 2)
    f_peer = lax.rem(d_peer + 2, 4)
    outs = [pltpu.make_async_copy(heads.at[g], out_hbm.at[g], out_sem.at[i]) for i, g in enumerate((s, x_peer, d_peer, f_peer))]
    outs[0].start()
    outs[1].start()
    for u, unit in enumerate(units):
        copy_of('d', d_peer, u, *unit).wait_recv()
    outs[2].start()
    for u, unit in enumerate(units):
        copy_of('f', f_peer, u, *unit).wait_recv()
    outs[3].start()
    for u, unit in enumerate(units):
        copy_of('x', s, u, *unit).wait_send()
        copy_of('d', s, u, *unit).wait_send()
        copy_of('f', x_peer, u, *unit).wait_send()
    for cp in outs:
        cp.wait()


def project(hidden, lengths, norm_gain, w_q, w_k, w_v, inv_freq):
    batch, dim = hidden.shape
    sp = 4
    n_head = w_q.shape[1] // sp // HEAD
    n_unit = n_head * HEAD // WIDE + 2
    vmem = pl.BlockSpec(memory_space=pltpu.VMEM)
    hbm = pl.BlockSpec(memory_space=pl.ANY)
    dma = pltpu.SemaphoreType.DMA
    return pl.pallas_call(
        qkv_kernel,
        out_shape=jax.ShapeDtypeStruct((sp, 2 + n_head, batch, HEAD), jnp.float32),
        in_specs=[pl.BlockSpec(memory_space=pltpu.SMEM), hbm, vmem, vmem, hbm, hbm, hbm],
        out_specs=hbm,
        scratch_shapes=[
            pltpu.VMEM((batch, dim), jnp.bfloat16),
            pltpu.VMEM((batch, dim), jnp.bfloat16),
            pltpu.VMEM((dim // HEAD, HEAD), jnp.float32),
            pltpu.VMEM((2, batch, HEAD), jnp.float32),
            pltpu.VMEM((SLOTS, KT, WIDE), jnp.bfloat16),
            pltpu.VMEM((batch, WIDE), jnp.float32),
            pltpu.VMEM((sp, 2 + n_head, batch, HEAD), jnp.float32),
            dma, dma((SLOTS,)), dma((SLOTS,)),
            dma((n_unit,)), dma((n_unit,)), dma((n_unit,)), dma((n_unit,)), dma((n_unit,)), dma((n_unit,)),
            dma((4,)),
        ],
        compiler_params=pltpu.CompilerParams(collective_id=0, has_side_effects=True, vmem_limit_bytes=60 * MIB),
        cost_estimate=pl.CostEstimate(flops=2 * batch * dim * (n_head + 2) * HEAD, bytes_accessed=2 * dim * (n_head + 2) * HEAD, transcendentals=0),
        name='qkv_exchange',
    )(lengths, hidden, norm_gain.reshape(dim // HEAD, HEAD), inv_freq.reshape(1, HEAD // 2), w_q, w_k, w_v)


def attend_kernel(len_ref, k_hbm, v_hbm, qkv_hbm, k_out, v_out, o_ref, ml_ref,
                  qkv, qkv_sem, kbuf, vbuf, slot_of, ml_rows, k_sem, v_sem, ko_sem, vo_sem):
    batch, rows, _ = k_hbm.shape
    n_kv = 4
    slots = rows // n_kv
    n_chunk = batch // SEQS
    n_unit = qkv.shape[0] // (n_kv * batch)
    group = n_unit - 2
    n_head = n_kv * group
    start = lax.axis_index('sp') * slots

    def in_copies(i):
        r = lax.rem(i, RING)
        seqs = pl.ds(i * SEQS, SEQS)
        return (pltpu.make_async_copy(k_hbm.at[seqs], kbuf.at[r], k_sem.at[r]),
                pltpu.make_async_copy(v_hbm.at[seqs], vbuf.at[r], v_sem.at[r]))

    def out_copies(i):
        r = lax.rem(i, RING)
        seqs = pl.ds(i * SEQS, SEQS)
        return (pltpu.make_async_copy(kbuf.at[r], k_out.at[seqs], ko_sem.at[r]),
                pltpu.make_async_copy(vbuf.at[r], v_out.at[seqs], vo_sem.at[r]))

    qkv_copy = pltpu.make_async_copy(qkv_hbm, qkv, qkv_sem)
    qkv_copy.start()
    for i in range(AHEAD):
        for cp in in_copies(i):
            cp.start()

    row = lax.broadcasted_iota(jnp.int32, (n_head, rows), 0)
    col = lax.broadcasted_iota(jnp.int32, (n_head, rows), 1)
    slot_of[...] = jnp.where(lax.rem(col, n_kv) == lax.div(row, group), lax.div(col, n_kv), 2 ** 30)
    win_row = lax.broadcasted_iota(jnp.int32, (16, HEAD), 0)
    lane = lax.broadcasted_iota(jnp.int32, (n_head, HEAD), 1)

    qkv_copy.wait()

    def new_rows(offset, b):
        four = qkv[pl.ds(offset * batch + b, n_kv, stride=n_unit * batch), :]
        return jnp.concatenate([four] * 4, axis=0).astype(jnp.bfloat16)

    def chunk_step(i, carry):
        r = lax.rem(i, RING)

        @pl.when(i + AHEAD < n_chunk)
        def _():
            @pl.when(i + AHEAD >= RING)
            def _():
                for cp in out_copies(i + AHEAD - RING):
                    cp.wait()
            for cp in in_copies(i + AHEAD):
                cp.start()

        for cp in in_copies(i):
            cp.wait()
        for j in range(SEQS):
            b = i * SEQS + j
            pos = len_ref[b] - start
            held = jnp.clip(pos, 0, slots - 1)
            window = pl.ds(pl.multiple_of(lax.div(held, 4) * 16, 16), 16)
            pick = lax.div(win_row, n_kv) == jnp.where(held == pos, lax.rem(held, 4), -1)
            kbuf[r, j, window, :] = jnp.where(pick, new_rows(0, b), kbuf[r, j, window, :])
            vbuf[r, j, window, :] = jnp.where(pick, new_rows(1, b), vbuf[r, j, window, :])
        for cp in out_copies(i):
            cp.start()
        def scores_of(j):
            b = i * SEQS + j
            q = jnp.concatenate([qkv[pl.ds((g * n_unit + 2) * batch + b, group, stride=batch), :] for g in range(n_kv)], axis=0)
            return lax.dot_general(q.astype(jnp.bfloat16), kbuf[r, j], (((1,), (1,)), ((), ())), preferred_element_type=jnp.float32)

        def softmax_of(j, scores):
            valid = slot_of[...] <= len_ref[i * SEQS + j] - start
            scores = jnp.where(valid, scores, MASKED)
            top = jnp.max(scores, axis=1, keepdims=True)
            weights = jnp.where(valid, jnp.exp((scores - top) * SCALE), 0.0)
            return weights.astype(jnp.bfloat16), top, jnp.sum(weights, axis=1, keepdims=True)

        def finish(j, weights, top, total):
            b = i * SEQS + j
            o_ref[pl.ds(b, n_head, stride=batch), :] = jnp.dot(weights, vbuf[r, j], preferred_element_type=jnp.float32)
            ml_rows[pl.ds(b, n_head, stride=batch), :] = jnp.where(lane < n_head, top * SCALE, total)

        sc = [scores_of(j) for j in range(SEQS)]
        sm = [softmax_of(j, sc[j]) for j in range(SEQS)]
        for j in range(SEQS):
            finish(j, *sm[j])
        return carry

    lax.fori_loop(0, n_chunk, chunk_step, 0)
    out_lane = lax.broadcasted_iota(jnp.int32, (batch, HEAD), 1)

    def gather_step(h, acc):
        mine = lax.rem(out_lane, n_head) == h
        return jnp.where(mine, ml_rows[pl.ds(pl.multiple_of(h * batch, 8), batch), :], acc)

    ml_ref[...] = lax.fori_loop(0, n_head, gather_step, jnp.zeros((batch, HEAD), jnp.float32))

    def drain(i, carry):
        for cp in out_copies(i):
            cp.wait()
        return carry

    lax.fori_loop(n_chunk - RING, n_chunk, drain, 0)


def attend(qkv, lengths, k_cache, v_cache):
    batch, slots, n_kv, head = k_cache.shape
    rows = slots * n_kv
    n_head = n_kv * (qkv.shape[1] - 2)
    flat = (batch, rows, head)
    smem = pl.BlockSpec(memory_space=pltpu.SMEM)
    vmem = pl.BlockSpec(memory_space=pltpu.VMEM)
    hbm = pl.BlockSpec(memory_space=pl.ANY)
    dma = pltpu.SemaphoreType.DMA((RING,))
    k_new, v_new, out, ml = pl.pallas_call(
        attend_kernel,
        out_shape=(jax.ShapeDtypeStruct(flat, jnp.bfloat16), jax.ShapeDtypeStruct(flat, jnp.bfloat16),
                   jax.ShapeDtypeStruct((n_head * batch, head), jnp.float32), jax.ShapeDtypeStruct((batch, head), jnp.float32)),
        in_specs=[smem, hbm, hbm, hbm],
        out_specs=(hbm, hbm, vmem, vmem),
        scratch_shapes=[
            pltpu.VMEM((qkv.shape[0] * qkv.shape[1] * batch, head), jnp.float32), pltpu.SemaphoreType.DMA,
            pltpu.VMEM((RING, SEQS, rows, head), jnp.bfloat16),
            pltpu.VMEM((RING, SEQS, rows, head), jnp.bfloat16),
            pltpu.VMEM((n_head, rows), jnp.int32),
            pltpu.VMEM((n_head * batch, head), jnp.float32),
            dma, dma, dma, dma,
        ],
        compiler_params=pltpu.CompilerParams(vmem_limit_bytes=50 * MIB),
        cost_estimate=pl.CostEstimate(flops=4 * batch * n_head * rows * head, bytes_accessed=8 * batch * rows * head, transcendentals=0),
        name='attend_local',
    )(lengths, k_cache.reshape(flat), v_cache.reshape(flat), qkv.reshape(-1, head))
    return k_new.reshape(k_cache.shape), v_new.reshape(v_cache.shape), out, ml


def combine_kernel(own, ml_ref, hid_hbm, wo, ybf,
                   other, ml_in, ml_chip, gates, mine, x_out, x_in, d_out, d_in, obf, hid, wbuf,
                   part, part_in, fin, fin_x, fin_d, fin_f,
                   hid_sem, w_sem, ml_send, ml_recv, o_send, o_recv, x_send, x_recv, d_send, d_recv,
                   p_send, p_recv, fx_send, fx_recv, fd_send, fd_recv, ff_send, ff_recv):
    n_head, batch, _ = own.shape
    rows = batch // 2
    half = n_head // 2
    n_piece = half // PIECE
    n_k = wo.shape[0] // OUT_K
    cols = wo.shape[1] // 2
    n_col = cols // OUT_W
    n_tile = n_col * n_k
    tp = lax.axis_index('tp')
    s = lax.axis_index('sp')
    x = lax.div(s, 2)
    c = lax.rem(s, 2)
    x_peer = lax.rem(s + 2, 4)
    d_peer = s + 1 - 2 * c
    my_rows = pl.ds(pl.multiple_of(x * rows, 16), rows)
    peer_rows = pl.ds(pl.multiple_of((1 - x) * rows, 16), rows)

    def remote(src, dst, send_sem, recv_sem, peer):
        device = {'sp': peer} if peer is not None else {'tp': 1 - tp}
        return pltpu.make_async_remote_copy(src, dst, send_sem, recv_sem, device_id=device, device_id_type=MESH_ID)

    def w_copy(t):
        lanes = pl.ds(pl.multiple_of(c * cols + lax.div(t, n_k) * OUT_W, OUT_W), OUT_W)
        depth = pl.ds(pl.multiple_of(lax.rem(t, n_k) * OUT_K, OUT_K), OUT_K)
        slot = lax.rem(t, OUT_SLOTS)
        return pltpu.make_async_copy(wo.at[depth, lanes], wbuf.at[slot], w_sem.at[slot])

    hid_copy = pltpu.make_async_copy(hid_hbm.at[my_rows, pl.ds(pl.multiple_of(c * cols, cols), cols)], hid, hid_sem)
    hid_copy.start()
    for t in range(OUT_SLOTS):
        w_copy(t).start(priority=1)

    barrier = pltpu.get_barrier_semaphore()
    for device in ({'sp': x_peer}, {'sp': d_peer}, {'tp': 1 - tp}):
        pl.semaphore_signal(barrier, inc=1, device_id=device, device_id_type=MESH_ID)
    pl.semaphore_wait(barrier, 3)

    ml_partner = remote(ml_ref, ml_in.at[0], ml_send.at[0], ml_recv.at[0], d_peer)
    ml_partner.start()

    def o_copy(p):
        return remote(own.at[pl.ds((1 - c) * half + p * PIECE, PIECE)], other.at[pl.ds(p * PIECE, PIECE)], o_send.at[p], o_recv.at[p], d_peer)

    for p in range(n_piece):
        o_copy(p).start()

    lane = lax.broadcasted_iota(jnp.int32, (batch, HEAD), 1)

    def merge_stats(first, second):
        top = jnp.maximum(first, second)
        factors = [jnp.exp(jnp.where(lane < n_head, m - top, 0.0)) for m in (first, second)]
        total = functools.reduce(jnp.add, [f * pltpu.roll(m, n_head, 1) for f, m in zip(factors, (first, second))])
        return top, factors, total

    def local_heads(per_head):
        return jnp.where(c == 0, per_head, pltpu.roll(per_head, HEAD - half, 1))

    ml_partner.wait()
    top, factors, total = merge_stats(ml_ref[...], ml_in[0])
    ml_chip[...] = jnp.where(lane < n_head, top, pltpu.roll(total, n_head, 1))
    for i in range(2):
        gates[i] = local_heads(factors[i])
    ml_x = remote(ml_chip, ml_in.at[1], ml_send.at[1], ml_recv.at[1], x_peer)

    def x_copy(p):
        part_of = pl.ds(p * PIECE, PIECE)
        return remote(x_out.at[part_of], x_in.at[part_of], x_send.at[p], x_recv.at[p], x_peer)

    def weigh(p, which):
        mine_gate = gates[0, which, :]
        other_gate = gates[1, which, :]
        out = []
        for h in range(PIECE):
            i = p * PIECE + h
            out.append(mine_gate[:, h:h + 1] * own[c * half + i, which, :] + other_gate[:, h:h + 1] * other[i, which, :])
        return out

    def mix_step(p, carry):
        o_copy(p).wait_recv()
        for h, val in enumerate(weigh(p, peer_rows)):
            x_out[p * PIECE + h] = val
        x_copy(p).start()

        @pl.when(p == 0)
        def _():
            ml_x.start()

        for h, val in enumerate(weigh(p, my_rows)):
            mine[p * PIECE + h] = val
        gates[0] = pltpu.roll(gates[0], HEAD - PIECE, 1)
        gates[1] = pltpu.roll(gates[1], HEAD - PIECE, 1)
        return carry

    lax.fori_loop(0, n_piece, mix_step, 0)
    ml_x.wait()
    top, factors, total = merge_stats(ml_chip[...], ml_in[1])
    for i in range(2):
        gates[i] = local_heads(factors[i] / total)

    def d_copy(p):
        part_of = pl.ds(p * PIECE, PIECE)
        return remote(d_out.at[part_of], d_in.at[part_of], d_send.at[p], d_recv.at[p], d_peer)

    def head_lanes(h):
        return pl.ds(pl.multiple_of(h * HEAD, HEAD), HEAD)

    def merge_step(p, carry):
        x_copy(p).wait_recv()
        mine_gate = gates[0, my_rows, :]
        in_gate = gates[1, my_rows, :]
        for h in range(PIECE):
            i = p * PIECE + h
            val = (mine_gate[:, h:h + 1] * mine[i] + in_gate[:, h:h + 1] * x_in[i]).astype(jnp.bfloat16)
            obf[:, head_lanes(c * half + i)] = val
            d_out[i] = val.astype(jnp.float32)
        d_copy(p).start()
        gates[0] = pltpu.roll(gates[0], HEAD - PIECE, 1)
        gates[1] = pltpu.roll(gates[1], HEAD - PIECE, 1)
        return carry

    lax.fori_loop(0, n_piece, merge_step, 0)

    def spread_step(p, carry):
        d_copy(p).wait_recv()
        for h in range(PIECE):
            i = p * PIECE + h
            obf[:, head_lanes((1 - c) * half + i)] = d_in[i].astype(jnp.bfloat16)
        return carry

    lax.fori_loop(0, n_piece, spread_step, 0)
    hid_copy.wait()

    def p_copy(j):
        return remote(part.at[j], part_in.at[j], p_send.at[j], p_recv.at[j], None)

    def fx_copy(j):
        return remote(fin.at[j], fin_x.at[j], fx_send.at[j], fx_recv.at[j], x_peer)

    def fd_copy(j):
        return remote(fin.at[j], fin_d.at[j], fd_send.at[j], fd_recv.at[j], d_peer)

    def ff_copy(j):
        return remote(fin_x.at[j], fin_f.at[j], ff_send.at[j], ff_recv.at[j], d_peer)

    def lanes_of(j, core):
        return pl.ds(pl.multiple_of(core * cols + j * OUT_W, OUT_W), OUT_W)

    def finish(j):
        p_copy(j).wait_recv()
        lane = pl.ds(pl.multiple_of(j * OUT_W, OUT_W), OUT_W)
        val = (hid[:, lane].astype(jnp.float32) + (part[j] + part_in[j])).astype(jnp.bfloat16)
        ybf[my_rows, lanes_of(j, c)] = val
        fin[j] = val.astype(jnp.float32)
        fx_copy(j).start()
        fd_copy(j).start()

    def pass_on(j):
        fx_copy(j).wait_recv()
        ff_copy(j).start()
        ybf[peer_rows, lanes_of(j, c)] = fin_x[j].astype(jnp.bfloat16)
        fd_copy(j).wait_recv()
        ybf[my_rows, lanes_of(j, 1 - c)] = fin_d[j].astype(jnp.bfloat16)

    def deliver(j):
        ff_copy(j).wait_recv()
        ybf[peer_rows, lanes_of(j, 1 - c)] = fin_f[j].astype(jnp.bfloat16)

    lags = (4, 8, 10)

    def col_step(j, carry):
        @pl.when(j < n_col)
        def _():
            acc = None
            for k in range(n_k):
                t = j * n_k + k
                w_copy(t).wait()
                term = jnp.dot(obf[:, k * OUT_K:(k + 1) * OUT_K], wbuf[lax.rem(t, OUT_SLOTS)], preferred_element_type=jnp.float32)
                acc = term if acc is None else acc + term

                @pl.when(t + OUT_SLOTS < n_tile)
                def _():
                    w_copy(t + OUT_SLOTS).start(priority=1)
            part[j] = acc
            p_copy(j).start()

        for lag, stage in zip(lags, (finish, pass_on, deliver)):
            @pl.when((j >= lag) & (j - lag < n_col))
            def _():
                stage(j - lag)
        return carry

    lax.fori_loop(0, n_col + lags[-1], col_step, 0)

    for p in range(n_piece):
        o_copy(p).wait_send()
        x_copy(p).wait_send()
        d_copy(p).wait_send()

    def drain(j, carry):
        p_copy(j).wait_send()
        fx_copy(j).wait_send()
        fd_copy(j).wait_send()
        ff_copy(j).wait_send()
        return carry

    lax.fori_loop(0, n_col, drain, 0)


def combine(out, ml, hidden, w_o):
    batch, dim = hidden.shape
    n_head = out.shape[0] // batch
    rows = batch // 2
    half = n_head // 2
    n_piece = half // PIECE
    n_col = dim // 2 // OUT_W
    vmem = pl.BlockSpec(memory_space=pltpu.VMEM)
    hbm = pl.BlockSpec(memory_space=pl.ANY)
    dma = pltpu.SemaphoreType.DMA
    f32 = jnp.float32
    quad = pltpu.VMEM((half, rows, HEAD), f32)
    tiles = pltpu.VMEM((n_col, rows, OUT_W), f32)
    return pl.pallas_call(
        combine_kernel,
        out_shape=jax.ShapeDtypeStruct((batch, dim), jnp.bfloat16),
        in_specs=[vmem, vmem, hbm, hbm],
        out_specs=vmem,
        scratch_shapes=[
            pltpu.VMEM((half, batch, HEAD), f32),
            pltpu.VMEM((2, batch, HEAD), f32), pltpu.VMEM((batch, HEAD), f32), pltpu.VMEM((2, batch, HEAD), f32),
            quad, quad, quad, quad, quad,
            pltpu.VMEM((rows, n_head * HEAD), jnp.bfloat16), pltpu.VMEM((rows, dim // 2), jnp.bfloat16),
            pltpu.VMEM((OUT_SLOTS, OUT_K, OUT_W), jnp.bfloat16),
            tiles, tiles, tiles, tiles, tiles, tiles,
            dma, dma((OUT_SLOTS,)), dma((2,)), dma((2,)),
            dma((n_piece,)), dma((n_piece,)), dma((n_piece,)), dma((n_piece,)), dma((n_piece,)), dma((n_piece,)),
            dma((n_col,)), dma((n_col,)), dma((n_col,)), dma((n_col,)), dma((n_col,)), dma((n_col,)), dma((n_col,)), dma((n_col,)),
        ],
        compiler_params=pltpu.CompilerParams(collective_id=1, has_side_effects=True, vmem_limit_bytes=46 * MIB),
        cost_estimate=pl.CostEstimate(flops=batch * dim * n_head * HEAD, bytes_accessed=dim * n_head * HEAD, transcendentals=0),
        name='combine_project',
    )(out.reshape(n_head, batch, HEAD), ml, hidden, w_o)


def device_step(hidden, lengths, k_cache, v_cache, norm_gain, w_q, w_k, w_v, w_o, inv_freq):
    qkv = project(hidden, lengths, norm_gain, w_q, w_k, w_v, inv_freq)
    k_new, v_new, out, ml = attend(qkv, lengths, k_cache, v_cache)
    return combine(out, ml, hidden, w_o), k_new, v_new


def solution(mesh):
    cache_spec = P('dp', 'sp', 'tp', None)
    in_specs = (P('dp', None), P('dp'), cache_spec, cache_spec, P(None), P(None, 'tp'), P(None, 'tp'), P(None, 'tp'), P('tp', None), P(None))
    out_specs = (P('dp', None), cache_spec, cache_spec)
    return jax.shard_map(device_step, mesh=mesh, in_specs=in_specs, out_specs=out_specs, check_vma=False)
```

```python
import functools

import jax
import jax.numpy as jnp
from jax import lax
from jax.experimental import pallas as pl
from jax.experimental.pallas import tpu as pltpu
from jax.sharding import PartitionSpec as P

NORM_EPS = 1e-5
HEAD = 128
KT = 2048
WIDE = 512
SLOTS = 16
MIB = 2 ** 20
MESH_ID = pl.DeviceIdType.MESH
SEQS = 16
RING = 4
AHEAD = 2
MASKED = -3e38
SCALE = HEAD ** -0.5
OUT_K = 8192
OUT_W = 256
OUT_SLOTS = 6
PIECE = 4


def rope(vec, cos_full, sin_signed):
    rounded = vec.astype(jnp.bfloat16).astype(jnp.float32)
    rotated = rounded * cos_full + pltpu.roll(rounded, 64, 1) * sin_signed
    return rotated.astype(jnp.bfloat16).astype(jnp.float32)


def qkv_kernel(len_ref, hid_hbm, gain_ref, freq_ref, wq, wk, wv, out_hbm,
               hid, normed, gain, trig, wbuf, acc, heads, hid_sem, w_sem,
               x_send, x_recv, d_send, d_recv, f_send, f_recv, out_sem):
    batch, dim = hid.shape
    n_k = dim // KT
    n_head = heads.shape[1] - 2
    cols = n_head * HEAD
    n_wide = cols // WIDE - 1
    half = WIDE // 2
    t_wide = n_k
    t_tail = t_wide + n_wide * n_k
    t_end = t_tail + 2 * n_k
    s = lax.axis_index('sp')
    x_peer = lax.rem(s + 2, 4)
    d_peer = s + 1 - 2 * lax.rem(s, 2)

    units = [(0, 2)] + [(2 + 4 * u, 4) for u in range(n_wide)] + [(2 + 4 * n_wide, 2), (4 + 4 * n_wide, 2)]

    def slot_of(t):
        return lax.rem(t, SLOTS)

    def rows_of(k):
        return pl.ds(pl.multiple_of(k * KT, KT), KT)

    is_key = s < 2

    def kv_copy(source, t):
        lanes = pl.ds(pl.multiple_of(lax.rem(s, 2) * half, half), half)
        return pltpu.make_async_copy(source.at[rows_of(t), lanes], wbuf.at[slot_of(t), :, pl.ds(0, half)], w_sem.at[slot_of(t)])

    def wide_copy(t):
        i = t - t_wide
        lanes = pl.ds(pl.multiple_of(s * cols + lax.div(i, n_k) * WIDE, WIDE), WIDE)
        return pltpu.make_async_copy(wq.at[rows_of(lax.rem(i, n_k)), lanes], wbuf.at[slot_of(t)], w_sem.at[slot_of(t)])

    def tail_copy(t):
        i = t - t_tail
        lanes = pl.ds(pl.multiple_of(s * cols + n_wide * WIDE + lax.div(i, n_k) * half, half), half)
        return pltpu.make_async_copy(wq.at[rows_of(lax.rem(i, n_k)), lanes], wbuf.at[slot_of(t), :, pl.ds(0, half)], w_sem.at[slot_of(t)])

    def start_tile(t):
        @pl.when(t < t_tail)
        def _():
            wide_copy(t).start(priority=1)

        @pl.when((t >= t_tail) & (t < t_end))
        def _():
            tail_copy(t).start(priority=1)

    hid_copy = pltpu.make_async_copy(hid_hbm, hid, hid_sem)
    hid_copy.start()
    for mine, source in ((is_key, wk), (jnp.logical_not(is_key), wv)):
        @pl.when(mine)
        def _():
            for t in range(n_k):
                kv_copy(source, t).start(priority=1)

    for t in range(n_k, SLOTS):
        wide_copy(t).start(priority=1)

    barrier = pltpu.get_barrier_semaphore()
    for peer in (x_peer, d_peer):
        pl.semaphore_signal(barrier, inc=1, device_id={'sp': peer}, device_id_type=MESH_ID)

    freq = jnp.concatenate([freq_ref[...], freq_ref[...]], axis=1)

    def angle_step(b, carry):
        trig[0, pl.ds(b, 1), :] = len_ref[b].astype(jnp.float32) * freq
        return carry

    lax.fori_loop(0, batch, angle_step, 0)
    angles = trig[0]
    sin_full = jnp.sin(angles)
    lane = lax.broadcasted_iota(jnp.int32, sin_full.shape, 1)
    trig[1] = jnp.where(lane < 64, -sin_full, sin_full)
    trig[0] = jnp.cos(angles)
    gain[...] = gain_ref[...].astype(jnp.float32)

    hid_copy.wait()
    step = 512

    def sq_step(i, acc):
        x = hid[:, pl.ds(pl.multiple_of(i * step, step), step)].astype(jnp.float32)
        x = x * x
        for t in range(step // 128):
            acc = acc + x[:, t * 128:(t + 1) * 128]
        return acc

    sq = lax.fori_loop(0, dim // step, sq_step, jnp.zeros((batch, 128), jnp.float32))
    inv = lax.rsqrt(jnp.sum(sq, axis=1, keepdims=True) / dim + NORM_EPS)
    inv = jnp.broadcast_to(inv, (batch, 128))

    def norm_step(i, carry):
        for t in range(step // 128):
            sl = pl.ds(pl.multiple_of(i * step + t * 128, 128), 128)
            x = hid[:, sl].astype(jnp.float32)
            row = gain[pl.ds(i * (step // 128) + t, 1), :]
            normed[:, sl] = (x * inv * row).astype(jnp.bfloat16)
        return carry

    lax.fori_loop(0, dim // step, norm_step, 0)

    def copy_of(kind, group, u, start, size):
        send_sem, recv_sem, peer = {'x': (x_send, x_recv, x_peer), 'd': (d_send, d_recv, d_peer), 'f': (f_send, f_recv, d_peer)}[kind]
        part = heads.at[group, pl.ds(start, size)]
        return pltpu.make_async_remote_copy(part, part, send_sem.at[u], recv_sem.at[u], device_id={'sp': peer}, device_id_type=MESH_ID)

    def publish(u, start, size):
        copy_of('x', s, u, start, size).start()
        copy_of('d', s, u, start, size).start()

    def forward(u):
        copy_of('x', x_peer, u, *units[u]).wait_recv()
        copy_of('f', x_peer, u, *units[u]).start()

    def multiply(t, k, width):
        part = jnp.dot(normed[:, rows_of(k)], wbuf[slot_of(t), :, pl.ds(0, width)], preferred_element_type=jnp.float32)

        @pl.when(k == 0)
        def _():
            acc[:, pl.ds(0, width)] = part

        @pl.when(k > 0)
        def _():
            acc[:, pl.ds(0, width)] += part

    def kv_step(t, carry):
        kv_copy(wk, t).wait()
        multiply(t, t, half)
        start_tile(t + SLOTS)
        return carry

    lax.fori_loop(0, n_k, kv_step, 0)
    pl.semaphore_wait(barrier, 2)
    for h in range(2):
        vec = acc[:, h * HEAD:(h + 1) * HEAD]
        heads[s, h] = jnp.where(is_key, rope(vec, trig[0], trig[1]), vec.astype(jnp.bfloat16).astype(jnp.float32))
    publish(0, *units[0])

    def wide_step(i, carry):
        t = i + t_wide
        k = lax.rem(i, n_k)
        chunk = lax.div(i, n_k)
        wide_copy(t).wait()
        multiply(t, k, WIDE)
        start_tile(t + SLOTS)

        @pl.when(k == n_k - 1)
        def _():
            first = 2 + 4 * chunk
            for h in range(4):
                heads[s, first + h] = rope(acc[:, h * HEAD:(h + 1) * HEAD], trig[0], trig[1])
            publish(chunk + 1, first, 4)

        for u in range(n_wide - 1):
            @pl.when(i == (u + 1) * n_k + (3 if u else -3))
            def _():
                forward(u)
        return carry

    lax.fori_loop(0, n_wide * n_k, wide_step, 0)

    def tail_step(i, carry):
        t = i + t_tail
        k = lax.rem(i, n_k)
        chunk = lax.div(i, n_k)
        tail_copy(t).wait()
        multiply(t, k, half)
        start_tile(t + SLOTS)

        @pl.when(k == n_k - 1)
        def _():
            first = 2 + 4 * n_wide + 2 * chunk
            for h in range(2):
                heads[s, first + h] = rope(acc[:, h * HEAD:(h + 1) * HEAD], trig[0], trig[1])
            publish(chunk + n_wide + 1, first, 2)

        @pl.when(i == 5)
        def _():
            forward(n_wide - 1)
        return carry

    lax.fori_loop(0, 2 * n_k, tail_step, 0)
    forward(n_wide)
    forward(n_wide + 1)
    forward(n_wide + 2)
    f_peer = lax.rem(d_peer + 2, 4)
    outs = [pltpu.make_async_copy(heads.at[g], out_hbm.at[g], out_sem.at[i]) for i, g in enumerate((s, x_peer, d_peer, f_peer))]
    outs[0].start()
    outs[1].start()
    for u, unit in enumerate(units):
        copy_of('d', d_peer, u, *unit).wait_recv()
    outs[2].start()
    for u, unit in enumerate(units):
        copy_of('f', f_peer, u, *unit).wait_recv()
    outs[3].start()
    for u, unit in enumerate(units):
        copy_of('x', s, u, *unit).wait_send()
        copy_of('d', s, u, *unit).wait_send()
        copy_of('f', x_peer, u, *unit).wait_send()
    for cp in outs:
        cp.wait()


def project(hidden, lengths, norm_gain, w_q, w_k, w_v, inv_freq):
    batch, dim = hidden.shape
    sp = 4
    n_head = w_q.shape[1] // sp // HEAD
    n_unit = n_head * HEAD // WIDE + 2
    vmem = pl.BlockSpec(memory_space=pltpu.VMEM)
    hbm = pl.BlockSpec(memory_space=pl.ANY)
    dma = pltpu.SemaphoreType.DMA
    return pl.pallas_call(
        qkv_kernel,
        out_shape=jax.ShapeDtypeStruct((sp, 2 + n_head, batch, HEAD), jnp.float32),
        in_specs=[pl.BlockSpec(memory_space=pltpu.SMEM), hbm, vmem, vmem, hbm, hbm, hbm],
        out_specs=hbm,
        scratch_shapes=[
            pltpu.VMEM((batch, dim), jnp.bfloat16),
            pltpu.VMEM((batch, dim), jnp.bfloat16),
            pltpu.VMEM((dim // HEAD, HEAD), jnp.float32),
            pltpu.VMEM((2, batch, HEAD), jnp.float32),
            pltpu.VMEM((SLOTS, KT, WIDE), jnp.bfloat16),
            pltpu.VMEM((batch, WIDE), jnp.float32),
            pltpu.VMEM((sp, 2 + n_head, batch, HEAD), jnp.float32),
            dma, dma((SLOTS,)),
            dma((n_unit,)), dma((n_unit,)), dma((n_unit,)), dma((n_unit,)), dma((n_unit,)), dma((n_unit,)),
            dma((4,)),
        ],
        compiler_params=pltpu.CompilerParams(collective_id=0, has_side_effects=True, vmem_limit_bytes=60 * MIB),
        cost_estimate=pl.CostEstimate(flops=2 * batch * dim * (n_head + 2) * HEAD, bytes_accessed=2 * dim * (n_head + 2) * HEAD, transcendentals=0),
        name='qkv_exchange',
    )(lengths, hidden, norm_gain.reshape(dim // HEAD, HEAD), inv_freq.reshape(1, HEAD // 2), w_q, w_k, w_v)


def attend_kernel(len_ref, k_hbm, v_hbm, qkv_hbm, k_out, v_out, o_ref, ml_ref,
                  qkv, qkv_sem, kbuf, vbuf, slot_of, ml_rows, k_sem, v_sem, ko_sem, vo_sem):
    batch, rows, _ = k_hbm.shape
    n_kv = 4
    slots = rows // n_kv
    n_chunk = batch // SEQS
    n_unit = qkv.shape[0] // (n_kv * batch)
    group = n_unit - 2
    n_head = n_kv * group
    start = lax.axis_index('sp') * slots

    def in_copies(i):
        r = lax.rem(i, RING)
        seqs = pl.ds(i * SEQS, SEQS)
        return (pltpu.make_async_copy(k_hbm.at[seqs], kbuf.at[r], k_sem.at[r]),
                pltpu.make_async_copy(v_hbm.at[seqs], vbuf.at[r], v_sem.at[r]))

    def out_copies(i):
        r = lax.rem(i, RING)
        seqs = pl.ds(i * SEQS, SEQS)
        return (pltpu.make_async_copy(kbuf.at[r], k_out.at[seqs], ko_sem.at[r]),
                pltpu.make_async_copy(vbuf.at[r], v_out.at[seqs], vo_sem.at[r]))

    qkv_copy = pltpu.make_async_copy(qkv_hbm, qkv, qkv_sem)
    qkv_copy.start()
    for i in range(AHEAD):
        for cp in in_copies(i):
            cp.start()

    row = lax.broadcasted_iota(jnp.int32, (n_head, rows), 0)
    col = lax.broadcasted_iota(jnp.int32, (n_head, rows), 1)
    slot_of[...] = jnp.where(lax.rem(col, n_kv) == lax.div(row, group), lax.div(col, n_kv), 2 ** 30)
    win_row = lax.broadcasted_iota(jnp.int32, (16, HEAD), 0)
    lane = lax.broadcasted_iota(jnp.int32, (n_head, HEAD), 1)

    qkv_copy.wait()

    def new_rows(offset, b):
        pairs = [qkv[pl.ds((2 * offset + i) * n_unit * batch + b, 2, stride=batch), :] for i in range(2)]
        return jnp.concatenate(pairs * 4, axis=0).astype(jnp.bfloat16)

    def chunk_step(i, carry):
        r = lax.rem(i, RING)

        @pl.when(i + AHEAD < n_chunk)
        def _():
            @pl.when(i + AHEAD >= RING)
            def _():
                for cp in out_copies(i + AHEAD - RING):
                    cp.wait()
            for cp in in_copies(i + AHEAD):
                cp.start()

        for cp in in_copies(i):
            cp.wait()
        for j in range(SEQS):
            b = i * SEQS + j
            pos = len_ref[b] - start
            held = jnp.clip(pos, 0, slots - 1)
            window = pl.ds(pl.multiple_of(lax.div(held, 4) * 16, 16), 16)
            pick = lax.div(win_row, n_kv) == jnp.where(held == pos, lax.rem(held, 4), -1)
            kbuf[r, j, window, :] = jnp.where(pick, new_rows(0, b), kbuf[r, j, window, :])
            vbuf[r, j, window, :] = jnp.where(pick, new_rows(1, b), vbuf[r, j, window, :])
        for cp in out_copies(i):
            cp.start()
        def scores_of(j):
            b = i * SEQS + j
            q = jnp.concatenate([qkv[pl.ds((g * n_unit + 2) * batch + b, group, stride=batch), :] for g in range(n_kv)], axis=0)
            return lax.dot_general(q.astype(jnp.bfloat16), kbuf[r, j], (((1,), (1,)), ((), ())), preferred_element_type=jnp.float32)

        def softmax_of(j, scores):
            valid = slot_of[...] <= len_ref[i * SEQS + j] - start
            scores = jnp.where(valid, scores, MASKED)
            top = jnp.max(scores, axis=1, keepdims=True)
            weights = jnp.where(valid, jnp.exp((scores - top) * SCALE), 0.0)
            return weights.astype(jnp.bfloat16), top, jnp.sum(weights, axis=1, keepdims=True)

        def finish(j, weights, top, total):
            b = i * SEQS + j
            o_ref[pl.ds(b, n_head, stride=batch), :] = jnp.dot(weights, vbuf[r, j], preferred_element_type=jnp.float32)
            ml_rows[pl.ds(b, n_head, stride=batch), :] = jnp.where(lane < n_head, top * SCALE, total)

        sc = [scores_of(j) for j in range(SEQS)]
        sm = [softmax_of(j, sc[j]) for j in range(SEQS)]
        for j in range(SEQS):
            finish(j, *sm[j])
        return carry

    lax.fori_loop(0, n_chunk, chunk_step, 0)
    out_lane = lax.broadcasted_iota(jnp.int32, (batch, HEAD), 1)

    def gather_step(h, acc):
        mine = lax.rem(out_lane, n_head) == h
        return jnp.where(mine, ml_rows[pl.ds(pl.multiple_of(h * batch, 8), batch), :], acc)

    ml_ref[...] = lax.fori_loop(0, n_head, gather_step, jnp.zeros((batch, HEAD), jnp.float32))

    def drain(i, carry):
        for cp in out_copies(i):
            cp.wait()
        return carry

    lax.fori_loop(n_chunk - RING, n_chunk, drain, 0)


def attend(qkv, lengths, k_cache, v_cache):
    batch, slots, n_kv, head = k_cache.shape
    rows = slots * n_kv
    n_head = n_kv * (qkv.shape[1] - 2)
    flat = (batch, rows, head)
    smem = pl.BlockSpec(memory_space=pltpu.SMEM)
    vmem = pl.BlockSpec(memory_space=pltpu.VMEM)
    hbm = pl.BlockSpec(memory_space=pl.ANY)
    dma = pltpu.SemaphoreType.DMA((RING,))
    k_new, v_new, out, ml = pl.pallas_call(
        attend_kernel,
        out_shape=(jax.ShapeDtypeStruct(flat, jnp.bfloat16), jax.ShapeDtypeStruct(flat, jnp.bfloat16),
                   jax.ShapeDtypeStruct((n_head * batch, head), jnp.float32), jax.ShapeDtypeStruct((batch, head), jnp.float32)),
        in_specs=[smem, hbm, hbm, hbm],
        out_specs=(hbm, hbm, vmem, vmem),
        scratch_shapes=[
            pltpu.VMEM((qkv.shape[0] * qkv.shape[1] * batch, head), jnp.float32), pltpu.SemaphoreType.DMA,
            pltpu.VMEM((RING, SEQS, rows, head), jnp.bfloat16),
            pltpu.VMEM((RING, SEQS, rows, head), jnp.bfloat16),
            pltpu.VMEM((n_head, rows), jnp.int32),
            pltpu.VMEM((n_head * batch, head), jnp.float32),
            dma, dma, dma, dma,
        ],
        compiler_params=pltpu.CompilerParams(vmem_limit_bytes=50 * MIB),
        cost_estimate=pl.CostEstimate(flops=4 * batch * n_head * rows * head, bytes_accessed=8 * batch * rows * head, transcendentals=0),
        name='attend_local',
    )(lengths, k_cache.reshape(flat), v_cache.reshape(flat), qkv.reshape(-1, head))
    return k_new.reshape(k_cache.shape), v_new.reshape(v_cache.shape), out, ml


def combine_kernel(own, ml_ref, hid_hbm, wo, ybf,
                   other, ml_in, ml_chip, gates, mine, x_out, x_in, d_out, d_in, obf, hid, wbuf,
                   part, part_in, fin, fin_x, fin_d, fin_f,
                   hid_sem, w_sem, ml_send, ml_recv, o_send, o_recv, x_send, x_recv, d_send, d_recv,
                   p_send, p_recv, fx_send, fx_recv, fd_send, fd_recv, ff_send, ff_recv):
    n_head, batch, _ = own.shape
    rows = batch // 2
    half = n_head // 2
    n_piece = half // PIECE
    n_k = wo.shape[0] // OUT_K
    cols = wo.shape[1] // 2
    n_col = cols // OUT_W
    n_tile = n_col * n_k
    tp = lax.axis_index('tp')
    s = lax.axis_index('sp')
    x = lax.div(s, 2)
    c = lax.rem(s, 2)
    x_peer = lax.rem(s + 2, 4)
    d_peer = s + 1 - 2 * c
    my_rows = pl.ds(pl.multiple_of(x * rows, 16), rows)
    peer_rows = pl.ds(pl.multiple_of((1 - x) * rows, 16), rows)

    def remote(src, dst, send_sem, recv_sem, peer):
        device = {'sp': peer} if peer is not None else {'tp': 1 - tp}
        return pltpu.make_async_remote_copy(src, dst, send_sem, recv_sem, device_id=device, device_id_type=MESH_ID)

    def w_copy(t):
        lanes = pl.ds(pl.multiple_of(c * cols + lax.div(t, n_k) * OUT_W, OUT_W), OUT_W)
        depth = pl.ds(pl.multiple_of(lax.rem(t, n_k) * OUT_K, OUT_K), OUT_K)
        slot = lax.rem(t, OUT_SLOTS)
        return pltpu.make_async_copy(wo.at[depth, lanes], wbuf.at[slot], w_sem.at[slot])

    hid_copy = pltpu.make_async_copy(hid_hbm.at[my_rows, pl.ds(pl.multiple_of(c * cols, cols), cols)], hid, hid_sem)
    hid_copy.start()
    for t in range(OUT_SLOTS):
        w_copy(t).start(priority=1)

    barrier = pltpu.get_barrier_semaphore()
    for device in ({'sp': x_peer}, {'sp': d_peer}, {'tp': 1 - tp}):
        pl.semaphore_signal(barrier, inc=1, device_id=device, device_id_type=MESH_ID)
    pl.semaphore_wait(barrier, 3)

    ml_partner = remote(ml_ref, ml_in.at[0], ml_send.at[0], ml_recv.at[0], d_peer)
    ml_partner.start()

    def o_copy(p):
        return remote(own.at[pl.ds((1 - c) * half + p * PIECE, PIECE)], other.at[pl.ds(p * PIECE, PIECE)], o_send.at[p], o_recv.at[p], d_peer)

    for p in range(n_piece):
        o_copy(p).start()

    lane = lax.broadcasted_iota(jnp.int32, (batch, HEAD), 1)

    def merge_stats(first, second):
        top = jnp.maximum(first, second)
        factors = [jnp.exp(jnp.where(lane < n_head, m - top, 0.0)) for m in (first, second)]
        total = functools.reduce(jnp.add, [f * pltpu.roll(m, n_head, 1) for f, m in zip(factors, (first, second))])
        return top, factors, total

    def local_heads(per_head):
        return jnp.where(c == 0, per_head, pltpu.roll(per_head, HEAD - half, 1))

    ml_partner.wait()
    top, factors, total = merge_stats(ml_ref[...], ml_in[0])
    ml_chip[...] = jnp.where(lane < n_head, top, pltpu.roll(total, n_head, 1))
    for i in range(2):
        gates[i] = local_heads(factors[i])
    ml_x = remote(ml_chip, ml_in.at[1], ml_send.at[1], ml_recv.at[1], x_peer)

    def x_copy(p):
        part_of = pl.ds(p * PIECE, PIECE)
        return remote(x_out.at[part_of], x_in.at[part_of], x_send.at[p], x_recv.at[p], x_peer)

    def weigh(p, which):
        mine_gate = gates[0, which, :]
        other_gate = gates[1, which, :]
        out = []
        for h in range(PIECE):
            i = p * PIECE + h
            out.append(mine_gate[:, h:h + 1] * own[c * half + i, which, :] + other_gate[:, h:h + 1] * other[i, which, :])
        return out

    def mix_step(p, carry):
        o_copy(p).wait_recv()
        for h, val in enumerate(weigh(p, peer_rows)):
            x_out[p * PIECE + h] = val
        x_copy(p).start()

        @pl.when(p == 0)
        def _():
            ml_x.start()

        for h, val in enumerate(weigh(p, my_rows)):
            mine[p * PIECE + h] = val
        gates[0] = pltpu.roll(gates[0], HEAD - PIECE, 1)
        gates[1] = pltpu.roll(gates[1], HEAD - PIECE, 1)
        return carry

    lax.fori_loop(0, n_piece, mix_step, 0)
    ml_x.wait()
    top, factors, total = merge_stats(ml_chip[...], ml_in[1])
    for i in range(2):
        gates[i] = local_heads(factors[i] / total)

    def d_copy(p):
        part_of = pl.ds(p * PIECE, PIECE)
        return remote(d_out.at[part_of], d_in.at[part_of], d_send.at[p], d_recv.at[p], d_peer)

    def head_lanes(h):
        return pl.ds(pl.multiple_of(h * HEAD, HEAD), HEAD)

    def merge_step(p, carry):
        x_copy(p).wait_recv()
        mine_gate = gates[0, my_rows, :]
        in_gate = gates[1, my_rows, :]
        for h in range(PIECE):
            i = p * PIECE + h
            val = (mine_gate[:, h:h + 1] * mine[i] + in_gate[:, h:h + 1] * x_in[i]).astype(jnp.bfloat16)
            obf[:, head_lanes(c * half + i)] = val
            d_out[i] = val.astype(jnp.float32)
        d_copy(p).start()
        gates[0] = pltpu.roll(gates[0], HEAD - PIECE, 1)
        gates[1] = pltpu.roll(gates[1], HEAD - PIECE, 1)
        return carry

    lax.fori_loop(0, n_piece, merge_step, 0)

    def spread_step(p, carry):
        d_copy(p).wait_recv()
        for h in range(PIECE):
            i = p * PIECE + h
            obf[:, head_lanes((1 - c) * half + i)] = d_in[i].astype(jnp.bfloat16)
        return carry

    lax.fori_loop(0, n_piece, spread_step, 0)
    hid_copy.wait()

    def p_copy(j):
        return remote(part.at[j], part_in.at[j], p_send.at[j], p_recv.at[j], None)

    def fx_copy(j):
        return remote(fin.at[j], fin_x.at[j], fx_send.at[j], fx_recv.at[j], x_peer)

    def fd_copy(j):
        return remote(fin.at[j], fin_d.at[j], fd_send.at[j], fd_recv.at[j], d_peer)

    def ff_copy(j):
        return remote(fin_x.at[j], fin_f.at[j], ff_send.at[j], ff_recv.at[j], d_peer)

    def lanes_of(j, core):
        return pl.ds(pl.multiple_of(core * cols + j * OUT_W, OUT_W), OUT_W)

    def finish(j):
        p_copy(j).wait_recv()
        lane = pl.ds(pl.multiple_of(j * OUT_W, OUT_W), OUT_W)
        val = (hid[:, lane].astype(jnp.float32) + (part[j] + part_in[j])).astype(jnp.bfloat16)
        ybf[my_rows, lanes_of(j, c)] = val
        fin[j] = val.astype(jnp.float32)
        fx_copy(j).start()
        fd_copy(j).start()

    def pass_on(j):
        fx_copy(j).wait_recv()
        ff_copy(j).start()
        ybf[peer_rows, lanes_of(j, c)] = fin_x[j].astype(jnp.bfloat16)
        fd_copy(j).wait_recv()
        ybf[my_rows, lanes_of(j, 1 - c)] = fin_d[j].astype(jnp.bfloat16)

    def deliver(j):
        ff_copy(j).wait_recv()
        ybf[peer_rows, lanes_of(j, 1 - c)] = fin_f[j].astype(jnp.bfloat16)

    lags = (4, 8, 10)

    def col_step(j, carry):
        @pl.when(j < n_col)
        def _():
            acc = None
            for k in range(n_k):
                t = j * n_k + k
                w_copy(t).wait()
                term = jnp.dot(obf[:, k * OUT_K:(k + 1) * OUT_K], wbuf[lax.rem(t, OUT_SLOTS)], preferred_element_type=jnp.float32)
                acc = term if acc is None else acc + term

                @pl.when(t + OUT_SLOTS < n_tile)
                def _():
                    w_copy(t + OUT_SLOTS).start(priority=1)
            part[j] = acc
            p_copy(j).start()

        for lag, stage in zip(lags, (finish, pass_on, deliver)):
            @pl.when((j >= lag) & (j - lag < n_col))
            def _():
                stage(j - lag)
        return carry

    lax.fori_loop(0, n_col + lags[-1], col_step, 0)

    for p in range(n_piece):
        o_copy(p).wait_send()
        x_copy(p).wait_send()
        d_copy(p).wait_send()

    def drain(j, carry):
        p_copy(j).wait_send()
        fx_copy(j).wait_send()
        fd_copy(j).wait_send()
        ff_copy(j).wait_send()
        return carry

    lax.fori_loop(0, n_col, drain, 0)


def combine(out, ml, hidden, w_o):
    batch, dim = hidden.shape
    n_head = out.shape[0] // batch
    rows = batch // 2
    half = n_head // 2
    n_piece = half // PIECE
    n_col = dim // 2 // OUT_W
    vmem = pl.BlockSpec(memory_space=pltpu.VMEM)
    hbm = pl.BlockSpec(memory_space=pl.ANY)
    dma = pltpu.SemaphoreType.DMA
    f32 = jnp.float32
    quad = pltpu.VMEM((half, rows, HEAD), f32)
    tiles = pltpu.VMEM((n_col, rows, OUT_W), f32)
    return pl.pallas_call(
        combine_kernel,
        out_shape=jax.ShapeDtypeStruct((batch, dim), jnp.bfloat16),
        in_specs=[vmem, vmem, hbm, hbm],
        out_specs=vmem,
        scratch_shapes=[
            pltpu.VMEM((half, batch, HEAD), f32),
            pltpu.VMEM((2, batch, HEAD), f32), pltpu.VMEM((batch, HEAD), f32), pltpu.VMEM((2, batch, HEAD), f32),
            quad, quad, quad, quad, quad,
            pltpu.VMEM((rows, n_head * HEAD), jnp.bfloat16), pltpu.VMEM((rows, dim // 2), jnp.bfloat16),
            pltpu.VMEM((OUT_SLOTS, OUT_K, OUT_W), jnp.bfloat16),
            tiles, tiles, tiles, tiles, tiles, tiles,
            dma, dma((OUT_SLOTS,)), dma((2,)), dma((2,)),
            dma((n_piece,)), dma((n_piece,)), dma((n_piece,)), dma((n_piece,)), dma((n_piece,)), dma((n_piece,)),
            dma((n_col,)), dma((n_col,)), dma((n_col,)), dma((n_col,)), dma((n_col,)), dma((n_col,)), dma((n_col,)), dma((n_col,)),
        ],
        compiler_params=pltpu.CompilerParams(collective_id=1, has_side_effects=True, vmem_limit_bytes=46 * MIB),
        cost_estimate=pl.CostEstimate(flops=batch * dim * n_head * HEAD, bytes_accessed=dim * n_head * HEAD, transcendentals=0),
        name='combine_project',
    )(out.reshape(n_head, batch, HEAD), ml, hidden, w_o)


def device_step(hidden, lengths, k_cache, v_cache, norm_gain, w_q, w_k, w_v, w_o, inv_freq):
    qkv = project(hidden, lengths, norm_gain, w_q, w_k, w_v, inv_freq)
    k_new, v_new, out, ml = attend(qkv, lengths, k_cache, v_cache)
    return combine(out, ml, hidden, w_o), k_new, v_new


def solution(mesh):
    cache_spec = P('dp', 'sp', 'tp', None)
    in_specs = (P('dp', None), P('dp'), cache_spec, cache_spec, P(None), P(None, 'tp'), P(None, 'tp'), P(None, 'tp'), P('tp', None), P(None))
    out_specs = (P('dp', None), cache_spec, cache_spec)
    return jax.shard_map(device_step, mesh=mesh, in_specs=in_specs, out_specs=out_specs, check_vma=False)
```

```python
import functools

import jax
import jax.numpy as jnp
from jax import lax
from jax.experimental import pallas as pl
from jax.experimental.pallas import tpu as pltpu
from jax.sharding import PartitionSpec as P

NORM_EPS = 1e-5
HEAD = 128
KT = 2048
WIDE = 512
SLOTS = 16
MIB = 2 ** 20
MESH_ID = pl.DeviceIdType.MESH
SEQS = 16
RING = 4
AHEAD = 2
MASKED = -3e38
SCALE = HEAD ** -0.5
OUT_K = 8192
OUT_W = 256
OUT_SLOTS = 7
PIECE = 4


def rope(vec, cos_full, sin_signed):
    rounded = vec.astype(jnp.bfloat16).astype(jnp.float32)
    rotated = rounded * cos_full + pltpu.roll(rounded, 64, 1) * sin_signed
    return rotated.astype(jnp.bfloat16).astype(jnp.float32)


def qkv_kernel(len_ref, hid_hbm, gain_ref, freq_ref, wq, wk, wv, out_hbm,
               hid, normed, gain, trig, wbuf, acc, heads, hid_sem, w_sem,
               x_send, x_recv, d_send, d_recv, f_send, f_recv, out_sem):
    batch, dim = hid.shape
    n_k = dim // KT
    n_head = heads.shape[1] - 2
    cols = n_head * HEAD
    n_wide = cols // WIDE - 1
    half = WIDE // 2
    t_wide = n_k
    t_tail = t_wide + n_wide * n_k
    t_end = t_tail + 2 * n_k
    s = lax.axis_index('sp')
    x_peer = lax.rem(s + 2, 4)
    d_peer = s + 1 - 2 * lax.rem(s, 2)

    units = [(0, 2)] + [(2 + 4 * u, 4) for u in range(n_wide)] + [(2 + 4 * n_wide, 2), (4 + 4 * n_wide, 2)]

    def slot_of(t):
        return lax.rem(t, SLOTS)

    def rows_of(k):
        return pl.ds(pl.multiple_of(k * KT, KT), KT)

    is_key = s < 2

    def kv_copy(source, t):
        lanes = pl.ds(pl.multiple_of(lax.rem(s, 2) * half, half), half)
        return pltpu.make_async_copy(source.at[rows_of(t), lanes], wbuf.at[slot_of(t), :, pl.ds(0, half)], w_sem.at[slot_of(t)])

    def wide_copy(t):
        i = t - t_wide
        lanes = pl.ds(pl.multiple_of(s * cols + lax.div(i, n_k) * WIDE, WIDE), WIDE)
        return pltpu.make_async_copy(wq.at[rows_of(lax.rem(i, n_k)), lanes], wbuf.at[slot_of(t)], w_sem.at[slot_of(t)])

    def tail_copy(t):
        i = t - t_tail
        lanes = pl.ds(pl.multiple_of(s * cols + n_wide * WIDE + lax.div(i, n_k) * half, half), half)
        return pltpu.make_async_copy(wq.at[rows_of(lax.rem(i, n_k)), lanes], wbuf.at[slot_of(t), :, pl.ds(0, half)], w_sem.at[slot_of(t)])

    def start_tile(t):
        @pl.when(t < t_tail)
        def _():
            wide_copy(t).start(priority=1)

        @pl.when((t >= t_tail) & (t < t_end))
        def _():
            tail_copy(t).start(priority=1)

    hid_copy = pltpu.make_async_copy(hid_hbm, hid, hid_sem)
    hid_copy.start()
    for mine, source in ((is_key, wk), (jnp.logical_not(is_key), wv)):
        @pl.when(mine)
        def _():
            for t in range(n_k):
                kv_copy(source, t).start(priority=1)

    for t in range(n_k, SLOTS):
        wide_copy(t).start(priority=1)

    barrier = pltpu.get_barrier_semaphore()
    for peer in (x_peer, d_peer):
        pl.semaphore_signal(barrier, inc=1, device_id={'sp': peer}, device_id_type=MESH_ID)

    freq = jnp.concatenate([freq_ref[...], freq_ref[...]], axis=1)

    def angle_step(b, carry):
        trig[0, pl.ds(b, 1), :] = len_ref[b].astype(jnp.float32) * freq
        return carry

    lax.fori_loop(0, batch, angle_step, 0)
    angles = trig[0]
    sin_full = jnp.sin(angles)
    lane = lax.broadcasted_iota(jnp.int32, sin_full.shape, 1)
    trig[1] = jnp.where(lane < 64, -sin_full, sin_full)
    trig[0] = jnp.cos(angles)
    gain[...] = gain_ref[...].astype(jnp.float32)

    hid_copy.wait()
    step = 512

    def sq_step(i, acc):
        x = hid[:, pl.ds(pl.multiple_of(i * step, step), step)].astype(jnp.float32)
        x = x * x
        for t in range(step // 128):
            acc = acc + x[:, t * 128:(t + 1) * 128]
        return acc

    sq = lax.fori_loop(0, dim // step, sq_step, jnp.zeros((batch, 128), jnp.float32))
    inv = lax.rsqrt(jnp.sum(sq, axis=1, keepdims=True) / dim + NORM_EPS)
    inv = jnp.broadcast_to(inv, (batch, 128))

    def norm_step(i, carry):
        for t in range(step // 128):
            sl = pl.ds(pl.multiple_of(i * step + t * 128, 128), 128)
            x = hid[:, sl].astype(jnp.float32)
            row = gain[pl.ds(i * (step // 128) + t, 1), :]
            normed[:, sl] = (x * inv * row).astype(jnp.bfloat16)
        return carry

    lax.fori_loop(0, dim // step, norm_step, 0)

    def copy_of(kind, group, u, start, size):
        send_sem, recv_sem, peer = {'x': (x_send, x_recv, x_peer), 'd': (d_send, d_recv, d_peer), 'f': (f_send, f_recv, d_peer)}[kind]
        part = heads.at[group, pl.ds(start, size)]
        return pltpu.make_async_remote_copy(part, part, send_sem.at[u], recv_sem.at[u], device_id={'sp': peer}, device_id_type=MESH_ID)

    def publish(u, start, size):
        copy_of('x', s, u, start, size).start()
        copy_of('d', s, u, start, size).start()

    def forward(u):
        copy_of('x', x_peer, u, *units[u]).wait_recv()
        copy_of('f', x_peer, u, *units[u]).start()

    def multiply(t, k, width):
        part = jnp.dot(normed[:, rows_of(k)], wbuf[slot_of(t), :, pl.ds(0, width)], preferred_element_type=jnp.float32)

        @pl.when(k == 0)
        def _():
            acc[:, pl.ds(0, width)] = part

        @pl.when(k > 0)
        def _():
            acc[:, pl.ds(0, width)] += part

    def kv_step(t, carry):
        kv_copy(wk, t).wait()
        multiply(t, t, half)
        start_tile(t + SLOTS)
        return carry

    lax.fori_loop(0, n_k, kv_step, 0)
    pl.semaphore_wait(barrier, 2)
    for h in range(2):
        vec = acc[:, h * HEAD:(h + 1) * HEAD]
        heads[s, h] = jnp.where(is_key, rope(vec, trig[0], trig[1]), vec.astype(jnp.bfloat16).astype(jnp.float32))
    publish(0, *units[0])

    def wide_step(i, carry):
        t = i + t_wide
        k = lax.rem(i, n_k)
        chunk = lax.div(i, n_k)
        wide_copy(t).wait()
        multiply(t, k, WIDE)
        start_tile(t + SLOTS)

        @pl.when(k == n_k - 1)
        def _():
            first = 2 + 4 * chunk
            for h in range(4):
                heads[s, first + h] = rope(acc[:, h * HEAD:(h + 1) * HEAD], trig[0], trig[1])
            publish(chunk + 1, first, 4)

        for u in range(n_wide - 1):
            @pl.when(i == (u + 1) * n_k + (3 if u else -3))
            def _():
                forward(u)
        return carry

    lax.fori_loop(0, n_wide * n_k, wide_step, 0)

    def tail_step(i, carry):
        t = i + t_tail
        k = lax.rem(i, n_k)
        chunk = lax.div(i, n_k)
        tail_copy(t).wait()
        multiply(t, k, half)
        start_tile(t + SLOTS)

        @pl.when(k == n_k - 1)
        def _():
            first = 2 + 4 * n_wide + 2 * chunk
            for h in range(2):
                heads[s, first + h] = rope(acc[:, h * HEAD:(h + 1) * HEAD], trig[0], trig[1])
            publish(chunk + n_wide + 1, first, 2)

        @pl.when(i == 5)
        def _():
            forward(n_wide - 1)
        return carry

    lax.fori_loop(0, 2 * n_k, tail_step, 0)
    forward(n_wide)
    forward(n_wide + 1)
    forward(n_wide + 2)
    f_peer = lax.rem(d_peer + 2, 4)
    outs = [pltpu.make_async_copy(heads.at[g], out_hbm.at[g], out_sem.at[i]) for i, g in enumerate((s, x_peer, d_peer, f_peer))]
    outs[0].start()
    outs[1].start()
    for u, unit in enumerate(units):
        copy_of('d', d_peer, u, *unit).wait_recv()
    outs[2].start()
    for u, unit in enumerate(units):
        copy_of('f', f_peer, u, *unit).wait_recv()
    outs[3].start()
    for u, unit in enumerate(units):
        copy_of('x', s, u, *unit).wait_send()
        copy_of('d', s, u, *unit).wait_send()
        copy_of('f', x_peer, u, *unit).wait_send()
    for cp in outs:
        cp.wait()


def project(hidden, lengths, norm_gain, w_q, w_k, w_v, inv_freq):
    batch, dim = hidden.shape
    sp = 4
    n_head = w_q.shape[1] // sp // HEAD
    n_unit = n_head * HEAD // WIDE + 2
    vmem = pl.BlockSpec(memory_space=pltpu.VMEM)
    hbm = pl.BlockSpec(memory_space=pl.ANY)
    dma = pltpu.SemaphoreType.DMA
    return pl.pallas_call(
        qkv_kernel,
        out_shape=jax.ShapeDtypeStruct((sp, 2 + n_head, batch, HEAD), jnp.float32),
        in_specs=[pl.BlockSpec(memory_space=pltpu.SMEM), hbm, vmem, vmem, hbm, hbm, hbm],
        out_specs=hbm,
        scratch_shapes=[
            pltpu.VMEM((batch, dim), jnp.bfloat16),
            pltpu.VMEM((batch, dim), jnp.bfloat16),
            pltpu.VMEM((dim // HEAD, HEAD), jnp.float32),
            pltpu.VMEM((2, batch, HEAD), jnp.float32),
            pltpu.VMEM((SLOTS, KT, WIDE), jnp.bfloat16),
            pltpu.VMEM((batch, WIDE), jnp.float32),
            pltpu.VMEM((sp, 2 + n_head, batch, HEAD), jnp.float32),
            dma, dma((SLOTS,)),
            dma((n_unit,)), dma((n_unit,)), dma((n_unit,)), dma((n_unit,)), dma((n_unit,)), dma((n_unit,)),
            dma((4,)),
        ],
        compiler_params=pltpu.CompilerParams(collective_id=0, has_side_effects=True, vmem_limit_bytes=60 * MIB),
        cost_estimate=pl.CostEstimate(flops=2 * batch * dim * (n_head + 2) * HEAD, bytes_accessed=2 * dim * (n_head + 2) * HEAD, transcendentals=0),
        name='qkv_exchange',
    )(lengths, hidden, norm_gain.reshape(dim // HEAD, HEAD), inv_freq.reshape(1, HEAD // 2), w_q, w_k, w_v)


def attend_kernel(len_ref, k_hbm, v_hbm, qkv_hbm, k_out, v_out, o_ref, ml_ref,
                  qkv, qkv_sem, kbuf, vbuf, slot_of, ml_rows, k_sem, v_sem, ko_sem, vo_sem):
    batch, rows, _ = k_hbm.shape
    n_kv = 4
    slots = rows // n_kv
    n_chunk = batch // SEQS
    n_unit = qkv.shape[0] // (n_kv * batch)
    group = n_unit - 2
    n_head = n_kv * group
    start = lax.axis_index('sp') * slots

    def in_copies(i):
        r = lax.rem(i, RING)
        seqs = pl.ds(i * SEQS, SEQS)
        return (pltpu.make_async_copy(k_hbm.at[seqs], kbuf.at[r], k_sem.at[r]),
                pltpu.make_async_copy(v_hbm.at[seqs], vbuf.at[r], v_sem.at[r]))

    def out_copies(i):
        r = lax.rem(i, RING)
        seqs = pl.ds(i * SEQS, SEQS)
        return (pltpu.make_async_copy(kbuf.at[r], k_out.at[seqs], ko_sem.at[r]),
                pltpu.make_async_copy(vbuf.at[r], v_out.at[seqs], vo_sem.at[r]))

    qkv_copy = pltpu.make_async_copy(qkv_hbm, qkv, qkv_sem)
    qkv_copy.start()
    for i in range(AHEAD):
        for cp in in_copies(i):
            cp.start()

    row = lax.broadcasted_iota(jnp.int32, (n_head, rows), 0)
    col = lax.broadcasted_iota(jnp.int32, (n_head, rows), 1)
    slot_of[...] = jnp.where(lax.rem(col, n_kv) == lax.div(row, group), lax.div(col, n_kv), 2 ** 30)
    win_row = lax.broadcasted_iota(jnp.int32, (16, HEAD), 0)
    lane = lax.broadcasted_iota(jnp.int32, (n_head, HEAD), 1)

    qkv_copy.wait()

    def new_rows(offset, b):
        pairs = [qkv[pl.ds((2 * offset + i) * n_unit * batch + b, 2, stride=batch), :] for i in range(2)]
        return jnp.concatenate(pairs * 4, axis=0).astype(jnp.bfloat16)

    def chunk_step(i, carry):
        r = lax.rem(i, RING)

        @pl.when(i + AHEAD < n_chunk)
        def _():
            @pl.when(i + AHEAD >= RING)
            def _():
                for cp in out_copies(i + AHEAD - RING):
                    cp.wait()
            for cp in in_copies(i + AHEAD):
                cp.start()

        for cp in in_copies(i):
            cp.wait()
        for j in range(SEQS):
            b = i * SEQS + j
            pos = len_ref[b] - start
            held = jnp.clip(pos, 0, slots - 1)
            window = pl.ds(pl.multiple_of(lax.div(held, 4) * 16, 16), 16)
            pick = lax.div(win_row, n_kv) == jnp.where(held == pos, lax.rem(held, 4), -1)
            kbuf[r, j, window, :] = jnp.where(pick, new_rows(0, b), kbuf[r, j, window, :])
            vbuf[r, j, window, :] = jnp.where(pick, new_rows(1, b), vbuf[r, j, window, :])
        for cp in out_copies(i):
            cp.start()
        def scores_of(j):
            b = i * SEQS + j
            q = jnp.concatenate([qkv[pl.ds((g * n_unit + 2) * batch + b, group, stride=batch), :] for g in range(n_kv)], axis=0)
            return lax.dot_general(q.astype(jnp.bfloat16), kbuf[r, j], (((1,), (1,)), ((), ())), preferred_element_type=jnp.float32)

        def softmax_of(j, scores):
            valid = slot_of[...] <= len_ref[i * SEQS + j] - start
            scores = jnp.where(valid, scores, MASKED)
            top = jnp.max(scores, axis=1, keepdims=True)
            weights = jnp.where(valid, jnp.exp((scores - top) * SCALE), 0.0)
            return weights.astype(jnp.bfloat16), top, jnp.sum(weights, axis=1, keepdims=True)

        def finish(j, weights, top, total):
            b = i * SEQS + j
            o_ref[pl.ds(b, n_head, stride=batch), :] = jnp.dot(weights, vbuf[r, j], preferred_element_type=jnp.float32)
            ml_rows[pl.ds(b, n_head, stride=batch), :] = jnp.where(lane < n_head, top * SCALE, total)

        sc = [scores_of(j) for j in range(SEQS)]
        sm = [softmax_of(j, sc[j]) for j in range(SEQS)]
        for j in range(SEQS):
            finish(j, *sm[j])
        return carry

    lax.fori_loop(0, n_chunk, chunk_step, 0)
    out_lane = lax.broadcasted_iota(jnp.int32, (batch, HEAD), 1)

    def gather_step(h, acc):
        mine = lax.rem(out_lane, n_head) == h
        return jnp.where(mine, ml_rows[pl.ds(pl.multiple_of(h * batch, 8), batch), :], acc)

    ml_ref[...] = lax.fori_loop(0, n_head, gather_step, jnp.zeros((batch, HEAD), jnp.float32))

    def drain(i, carry):
        for cp in out_copies(i):
            cp.wait()
        return carry

    lax.fori_loop(n_chunk - RING, n_chunk, drain, 0)


def attend(qkv, lengths, k_cache, v_cache):
    batch, slots, n_kv, head = k_cache.shape
    rows = slots * n_kv
    n_head = n_kv * (qkv.shape[1] - 2)
    flat = (batch, rows, head)
    smem = pl.BlockSpec(memory_space=pltpu.SMEM)
    vmem = pl.BlockSpec(memory_space=pltpu.VMEM)
    hbm = pl.BlockSpec(memory_space=pl.ANY)
    dma = pltpu.SemaphoreType.DMA((RING,))
    k_new, v_new, out, ml = pl.pallas_call(
        attend_kernel,
        out_shape=(jax.ShapeDtypeStruct(flat, jnp.bfloat16), jax.ShapeDtypeStruct(flat, jnp.bfloat16),
                   jax.ShapeDtypeStruct((n_head * batch, head), jnp.float32), jax.ShapeDtypeStruct((batch, head), jnp.float32)),
        in_specs=[smem, hbm, hbm, hbm],
        out_specs=(hbm, hbm, vmem, vmem),
        scratch_shapes=[
            pltpu.VMEM((qkv.shape[0] * qkv.shape[1] * batch, head), jnp.float32), pltpu.SemaphoreType.DMA,
            pltpu.VMEM((RING, SEQS, rows, head), jnp.bfloat16),
            pltpu.VMEM((RING, SEQS, rows, head), jnp.bfloat16),
            pltpu.VMEM((n_head, rows), jnp.int32),
            pltpu.VMEM((n_head * batch, head), jnp.float32),
            dma, dma, dma, dma,
        ],
        compiler_params=pltpu.CompilerParams(vmem_limit_bytes=50 * MIB),
        cost_estimate=pl.CostEstimate(flops=4 * batch * n_head * rows * head, bytes_accessed=8 * batch * rows * head, transcendentals=0),
        name='attend_local',
    )(lengths, k_cache.reshape(flat), v_cache.reshape(flat), qkv.reshape(-1, head))
    return k_new.reshape(k_cache.shape), v_new.reshape(v_cache.shape), out, ml


def combine_kernel(own, ml_ref, hid_hbm, wo, ybf,
                   other, ml_in, ml_chip, gates, mine, x_out, x_in, d_in, obf, hid, wbuf,
                   part, part_in, fin_x, fin_d, fin_f,
                   hid_sem, w_sem, ml_send, ml_recv, o_send, o_recv, x_send, x_recv, d_send, d_recv,
                   p_send, p_recv, fx_send, fx_recv, fd_send, fd_recv, ff_send, ff_recv):
    n_head, batch, _ = own.shape
    rows = batch // 2
    half = n_head // 2
    n_piece = half // PIECE
    n_k = wo.shape[0] // OUT_K
    cols = wo.shape[1] // 2
    n_col = cols // OUT_W
    n_tile = n_col * n_k
    tp = lax.axis_index('tp')
    s = lax.axis_index('sp')
    x = lax.div(s, 2)
    c = lax.rem(s, 2)
    x_peer = lax.rem(s + 2, 4)
    d_peer = s + 1 - 2 * c
    my_rows = pl.ds(pl.multiple_of(x * rows, 16), rows)
    peer_rows = pl.ds(pl.multiple_of((1 - x) * rows, 16), rows)

    def remote(src, dst, send_sem, recv_sem, peer):
        device = {'sp': peer} if peer is not None else {'tp': 1 - tp}
        return pltpu.make_async_remote_copy(src, dst, send_sem, recv_sem, device_id=device, device_id_type=MESH_ID)

    def w_copy(t):
        lanes = pl.ds(pl.multiple_of(c * cols + lax.div(t, n_k) * OUT_W, OUT_W), OUT_W)
        depth = pl.ds(pl.multiple_of(lax.rem(t, n_k) * OUT_K, OUT_K), OUT_K)
        slot = lax.rem(t, OUT_SLOTS)
        return pltpu.make_async_copy(wo.at[depth, lanes], wbuf.at[slot], w_sem.at[slot])

    hid_copy = pltpu.make_async_copy(hid_hbm.at[my_rows, pl.ds(pl.multiple_of(c * cols, cols), cols)], hid, hid_sem)
    hid_copy.start()
    for t in range(OUT_SLOTS):
        w_copy(t).start(priority=1)

    barrier = pltpu.get_barrier_semaphore()
    for device in ({'sp': x_peer}, {'sp': d_peer}, {'tp': 1 - tp}):
        pl.semaphore_signal(barrier, inc=1, device_id=device, device_id_type=MESH_ID)
    pl.semaphore_wait(barrier, 3)

    ml_partner = remote(ml_ref, ml_in.at[0], ml_send.at[0], ml_recv.at[0], d_peer)
    ml_partner.start()

    def o_copy(p):
        return remote(own.at[pl.ds((1 - c) * half + p * PIECE, PIECE)], other.at[pl.ds(p * PIECE, PIECE)], o_send.at[p], o_recv.at[p], d_peer)

    for p in range(n_piece):
        o_copy(p).start()

    lane = lax.broadcasted_iota(jnp.int32, (batch, HEAD), 1)

    def merge_stats(first, second):
        top = jnp.maximum(first, second)
        factors = [jnp.exp(jnp.where(lane < n_head, m - top, 0.0)) for m in (first, second)]
        total = functools.reduce(jnp.add, [f * pltpu.roll(m, n_head, 1) for f, m in zip(factors, (first, second))])
        return top, factors, total

    def local_heads(per_head):
        return jnp.where(c == 0, per_head, pltpu.roll(per_head, HEAD - half, 1))

    ml_partner.wait()
    top, factors, total = merge_stats(ml_ref[...], ml_in[0])
    ml_chip[...] = jnp.where(lane < n_head, top, pltpu.roll(total, n_head, 1))
    for i in range(2):
        gates[i] = local_heads(factors[i])
    ml_x = remote(ml_chip, ml_in.at[1], ml_send.at[1], ml_recv.at[1], x_peer)

    def x_copy(p):
        part_of = pl.ds(p * PIECE, PIECE)
        return remote(x_out.at[part_of], x_in.at[part_of], x_send.at[p], x_recv.at[p], x_peer)

    def weigh(p, which):
        mine_gate = gates[0, which, :]
        other_gate = gates[1, which, :]
        out = []
        for h in range(PIECE):
            i = p * PIECE + h
            out.append(mine_gate[:, h:h + 1] * own[c * half + i, which, :] + other_gate[:, h:h + 1] * other[i, which, :])
        return out

    def mix_step(p, carry):
        o_copy(p).wait_recv()
        for h, val in enumerate(weigh(p, peer_rows)):
            x_out[p * PIECE + h] = val
        x_copy(p).start()

        @pl.when(p == 0)
        def _():
            ml_x.start()

        for h, val in enumerate(weigh(p, my_rows)):
            mine[p * PIECE + h] = val
        gates[0] = pltpu.roll(gates[0], HEAD - PIECE, 1)
        gates[1] = pltpu.roll(gates[1], HEAD - PIECE, 1)
        return carry

    lax.fori_loop(0, n_piece, mix_step, 0)
    ml_x.wait()
    top, factors, total = merge_stats(ml_chip[...], ml_in[1])
    for i in range(2):
        gates[i] = local_heads(factors[i] / total)

    def d_copy(p):
        part_of = pl.ds(p * PIECE, PIECE)
        return remote(mine.at[part_of], d_in.at[part_of], d_send.at[p], d_recv.at[p], d_peer)

    def head_lanes(h):
        return pl.ds(pl.multiple_of(h * HEAD, HEAD), HEAD)

    def merge_step(p, carry):
        x_copy(p).wait_recv()
        mine_gate = gates[0, my_rows, :]
        in_gate = gates[1, my_rows, :]
        for h in range(PIECE):
            i = p * PIECE + h
            val = (mine_gate[:, h:h + 1] * mine[i] + in_gate[:, h:h + 1] * x_in[i]).astype(jnp.bfloat16)
            obf[:, head_lanes(c * half + i)] = val
            mine[i] = val.astype(jnp.float32)
        d_copy(p).start()
        gates[0] = pltpu.roll(gates[0], HEAD - PIECE, 1)
        gates[1] = pltpu.roll(gates[1], HEAD - PIECE, 1)
        return carry

    lax.fori_loop(0, n_piece, merge_step, 0)

    def spread_step(p, carry):
        d_copy(p).wait_recv()
        for h in range(PIECE):
            i = p * PIECE + h
            obf[:, head_lanes((1 - c) * half + i)] = d_in[i].astype(jnp.bfloat16)
        return carry

    lax.fori_loop(0, n_piece, spread_step, 0)
    hid_copy.wait()

    def p_copy(j):
        return remote(part.at[j], part_in.at[j], p_send.at[j], p_recv.at[j], None)

    def fx_copy(j):
        return remote(part.at[j], fin_x.at[j], fx_send.at[j], fx_recv.at[j], x_peer)

    def fd_copy(j):
        return remote(part.at[j], fin_d.at[j], fd_send.at[j], fd_recv.at[j], d_peer)

    def ff_copy(j):
        return remote(fin_x.at[j], fin_f.at[j], ff_send.at[j], ff_recv.at[j], d_peer)

    def lanes_of(j, core):
        return pl.ds(pl.multiple_of(core * cols + j * OUT_W, OUT_W), OUT_W)

    def finish(j):
        p_copy(j).wait_recv()
        lane = pl.ds(pl.multiple_of(j * OUT_W, OUT_W), OUT_W)
        val = (hid[:, lane].astype(jnp.float32) + (part[j] + part_in[j])).astype(jnp.bfloat16)
        ybf[my_rows, lanes_of(j, c)] = val
        p_copy(j).wait_send()
        part[j] = val.astype(jnp.float32)
        fx_copy(j).start()
        fd_copy(j).start()

    def pass_on(j):
        fx_copy(j).wait_recv()
        ff_copy(j).start()
        ybf[peer_rows, lanes_of(j, c)] = fin_x[j].astype(jnp.bfloat16)
        fd_copy(j).wait_recv()
        ybf[my_rows, lanes_of(j, 1 - c)] = fin_d[j].astype(jnp.bfloat16)

    def deliver(j):
        ff_copy(j).wait_recv()
        ybf[peer_rows, lanes_of(j, 1 - c)] = fin_f[j].astype(jnp.bfloat16)

    lags = (4, 8, 10)

    def col_step(j, carry):
        @pl.when(j < n_col)
        def _():
            acc = None
            for k in range(n_k):
                t = j * n_k + k
                w_copy(t).wait()
                term = jnp.dot(obf[:, k * OUT_K:(k + 1) * OUT_K], wbuf[lax.rem(t, OUT_SLOTS)], preferred_element_type=jnp.float32)
                acc = term if acc is None else acc + term

                @pl.when(t + OUT_SLOTS < n_tile)
                def _():
                    w_copy(t + OUT_SLOTS).start(priority=1)
            part[j] = acc
            p_copy(j).start()

        for lag, stage in zip(lags, (finish, pass_on, deliver)):
            @pl.when((j >= lag) & (j - lag < n_col))
            def _():
                stage(j - lag)
        return carry

    lax.fori_loop(0, n_col + lags[-1], col_step, 0)

    for p in range(n_piece):
        o_copy(p).wait_send()
        x_copy(p).wait_send()
        d_copy(p).wait_send()

    def drain(j, carry):
        fx_copy(j).wait_send()
        fd_copy(j).wait_send()
        ff_copy(j).wait_send()
        return carry

    lax.fori_loop(0, n_col, drain, 0)


def combine(out, ml, hidden, w_o):
    batch, dim = hidden.shape
    n_head = out.shape[0] // batch
    rows = batch // 2
    half = n_head // 2
    n_piece = half // PIECE
    n_col = dim // 2 // OUT_W
    vmem = pl.BlockSpec(memory_space=pltpu.VMEM)
    hbm = pl.BlockSpec(memory_space=pl.ANY)
    dma = pltpu.SemaphoreType.DMA
    f32 = jnp.float32
    quad = pltpu.VMEM((half, rows, HEAD), f32)
    tiles = pltpu.VMEM((n_col, rows, OUT_W), f32)
    return pl.pallas_call(
        combine_kernel,
        out_shape=jax.ShapeDtypeStruct((batch, dim), jnp.bfloat16),
        in_specs=[vmem, vmem, hbm, hbm],
        out_specs=vmem,
        scratch_shapes=[
            pltpu.VMEM((half, batch, HEAD), f32),
            pltpu.VMEM((2, batch, HEAD), f32), pltpu.VMEM((batch, HEAD), f32), pltpu.VMEM((2, batch, HEAD), f32),
            quad, quad, quad, quad,
            pltpu.VMEM((rows, n_head * HEAD), jnp.bfloat16), pltpu.VMEM((rows, dim // 2), jnp.bfloat16),
            pltpu.VMEM((OUT_SLOTS, OUT_K, OUT_W), jnp.bfloat16),
            tiles, tiles, tiles, tiles, tiles,
            dma, dma((OUT_SLOTS,)), dma((2,)), dma((2,)),
            dma((n_piece,)), dma((n_piece,)), dma((n_piece,)), dma((n_piece,)), dma((n_piece,)), dma((n_piece,)),
            dma((n_col,)), dma((n_col,)), dma((n_col,)), dma((n_col,)), dma((n_col,)), dma((n_col,)), dma((n_col,)), dma((n_col,)),
        ],
        compiler_params=pltpu.CompilerParams(collective_id=1, has_side_effects=True, vmem_limit_bytes=46 * MIB),
        cost_estimate=pl.CostEstimate(flops=batch * dim * n_head * HEAD, bytes_accessed=dim * n_head * HEAD, transcendentals=0),
        name='combine_project',
    )(out.reshape(n_head, batch, HEAD), ml, hidden, w_o)


def device_step(hidden, lengths, k_cache, v_cache, norm_gain, w_q, w_k, w_v, w_o, inv_freq):
    qkv = project(hidden, lengths, norm_gain, w_q, w_k, w_v, inv_freq)
    k_new, v_new, out, ml = attend(qkv, lengths, k_cache, v_cache)
    return combine(out, ml, hidden, w_o), k_new, v_new


def solution(mesh):
    cache_spec = P('dp', 'sp', 'tp', None)
    in_specs = (P('dp', None), P('dp'), cache_spec, cache_spec, P(None), P(None, 'tp'), P(None, 'tp'), P(None, 'tp'), P('tp', None), P(None))
    out_specs = (P('dp', None), cache_spec, cache_spec)
    return jax.shard_map(device_step, mesh=mesh, in_specs=in_specs, out_specs=out_specs, check_vma=False)
```

```python
import functools

import jax
import jax.numpy as jnp
from jax import lax
from jax.experimental import pallas as pl
from jax.experimental.pallas import tpu as pltpu
from jax.sharding import PartitionSpec as P

NORM_EPS = 1e-5
HEAD = 128
KT = 2048
WIDE = 512
SLOTS = 16
MIB = 2 ** 20
MESH_ID = pl.DeviceIdType.MESH
SEQS = 16
RING = 4
AHEAD = 2
MASKED = -3e38
SCALE = HEAD ** -0.5
OUT_K = 8192
OUT_W = 256
OUT_SLOTS = 7
PIECE = 4


def rope(vec, cos_full, sin_signed):
    rounded = vec.astype(jnp.bfloat16).astype(jnp.float32)
    rotated = rounded * cos_full + pltpu.roll(rounded, 64, 1) * sin_signed
    return rotated.astype(jnp.bfloat16).astype(jnp.float32)


def qkv_kernel(len_ref, hid_hbm, gain_ref, freq_ref, wq, wk, wv, out_hbm,
               hid, normed, gain, trig, wbuf, acc, heads, hid_sem, w_sem,
               x_send, x_recv, d_send, d_recv, f_send, f_recv, out_sem):
    batch, dim = hid.shape
    n_k = dim // KT
    n_head = heads.shape[1] - 2
    cols = n_head * HEAD
    n_wide = cols // WIDE - 1
    half = WIDE // 2
    t_wide = n_k
    t_tail = t_wide + n_wide * n_k
    t_end = t_tail + 2 * n_k
    s = lax.axis_index('sp')
    x_peer = lax.rem(s + 2, 4)
    d_peer = s + 1 - 2 * lax.rem(s, 2)

    units = [(0, 2)] + [(2 + 4 * u, 4) for u in range(n_wide)] + [(2 + 4 * n_wide, 2), (4 + 4 * n_wide, 2)]

    def slot_of(t):
        return lax.rem(t, SLOTS)

    def rows_of(k):
        return pl.ds(pl.multiple_of(k * KT, KT), KT)

    is_key = s < 2

    def kv_copy(source, t):
        lanes = pl.ds(pl.multiple_of(lax.rem(s, 2) * half, half), half)
        return pltpu.make_async_copy(source.at[rows_of(t), lanes], wbuf.at[slot_of(t), :, pl.ds(0, half)], w_sem.at[slot_of(t)])

    def wide_copy(t):
        i = t - t_wide
        lanes = pl.ds(pl.multiple_of(s * cols + lax.div(i, n_k) * WIDE, WIDE), WIDE)
        return pltpu.make_async_copy(wq.at[rows_of(lax.rem(i, n_k)), lanes], wbuf.at[slot_of(t)], w_sem.at[slot_of(t)])

    def tail_copy(t):
        i = t - t_tail
        lanes = pl.ds(pl.multiple_of(s * cols + n_wide * WIDE + lax.div(i, n_k) * half, half), half)
        return pltpu.make_async_copy(wq.at[rows_of(lax.rem(i, n_k)), lanes], wbuf.at[slot_of(t), :, pl.ds(0, half)], w_sem.at[slot_of(t)])

    def start_tile(t):
        @pl.when(t < t_tail)
        def _():
            wide_copy(t).start(priority=1)

        @pl.when((t >= t_tail) & (t < t_end))
        def _():
            tail_copy(t).start(priority=1)

    hid_copy = pltpu.make_async_copy(hid_hbm, hid, hid_sem)
    hid_copy.start()
    for mine, source in ((is_key, wk), (jnp.logical_not(is_key), wv)):
        @pl.when(mine)
        def _():
            for t in range(n_k):
                kv_copy(source, t).start(priority=1)

    for t in range(n_k, SLOTS):
        wide_copy(t).start(priority=1)

    barrier = pltpu.get_barrier_semaphore()
    for peer in (x_peer, d_peer):
        pl.semaphore_signal(barrier, inc=1, device_id={'sp': peer}, device_id_type=MESH_ID)

    freq = jnp.concatenate([freq_ref[...], freq_ref[...]], axis=1)

    def angle_step(b, carry):
        trig[0, pl.ds(b, 1), :] = len_ref[b].astype(jnp.float32) * freq
        return carry

    lax.fori_loop(0, batch, angle_step, 0)
    angles = trig[0]
    sin_full = jnp.sin(angles)
    lane = lax.broadcasted_iota(jnp.int32, sin_full.shape, 1)
    trig[1] = jnp.where(lane < 64, -sin_full, sin_full)
    trig[0] = jnp.cos(angles)
    gain[...] = gain_ref[...].astype(jnp.float32)

    hid_copy.wait()
    step = 512

    def sq_step(i, acc):
        x = hid[:, pl.ds(pl.multiple_of(i * step, step), step)].astype(jnp.float32)
        x = x * x
        for t in range(step // 128):
            acc = acc + x[:, t * 128:(t + 1) * 128]
        return acc

    sq = lax.fori_loop(0, dim // step, sq_step, jnp.zeros((batch, 128), jnp.float32))
    inv = lax.rsqrt(jnp.sum(sq, axis=1, keepdims=True) / dim + NORM_EPS)
    inv = jnp.broadcast_to(inv, (batch, 128))

    def norm_step(i, carry):
        for t in range(step // 128):
            sl = pl.ds(pl.multiple_of(i * step + t * 128, 128), 128)
            x = hid[:, sl].astype(jnp.float32)
            row = gain[pl.ds(i * (step // 128) + t, 1), :]
            normed[:, sl] = (x * inv * row).astype(jnp.bfloat16)
        return carry

    lax.fori_loop(0, dim // step, norm_step, 0)

    def copy_of(kind, group, u, start, size):
        send_sem, recv_sem, peer = {'x': (x_send, x_recv, x_peer), 'd': (d_send, d_recv, d_peer), 'f': (f_send, f_recv, d_peer)}[kind]
        part = heads.at[group, pl.ds(start, size)]
        return pltpu.make_async_remote_copy(part, part, send_sem.at[u], recv_sem.at[u], device_id={'sp': peer}, device_id_type=MESH_ID)

    def publish(u, start, size):
        copy_of('x', s, u, start, size).start()
        copy_of('d', s, u, start, size).start()

    def forward(u):
        copy_of('x', x_peer, u, *units[u]).wait_recv()
        copy_of('f', x_peer, u, *units[u]).start()

    def multiply(t, k, width):
        part = jnp.dot(normed[:, rows_of(k)], wbuf[slot_of(t), :, pl.ds(0, width)], preferred_element_type=jnp.float32)

        @pl.when(k == 0)
        def _():
            acc[:, pl.ds(0, width)] = part

        @pl.when(k > 0)
        def _():
            acc[:, pl.ds(0, width)] += part

    def kv_step(t, carry):
        kv_copy(wk, t).wait()
        multiply(t, t, half)
        start_tile(t + SLOTS)
        return carry

    lax.fori_loop(0, n_k, kv_step, 0)
    pl.semaphore_wait(barrier, 2)
    for h in range(2):
        vec = acc[:, h * HEAD:(h + 1) * HEAD]
        heads[s, h] = jnp.where(is_key, rope(vec, trig[0], trig[1]), vec.astype(jnp.bfloat16).astype(jnp.float32))
    publish(0, *units[0])

    def wide_step(i, carry):
        t = i + t_wide
        k = lax.rem(i, n_k)
        chunk = lax.div(i, n_k)
        wide_copy(t).wait()
        multiply(t, k, WIDE)
        start_tile(t + SLOTS)

        @pl.when(k == n_k - 1)
        def _():
            first = 2 + 4 * chunk
            for h in range(4):
                heads[s, first + h] = rope(acc[:, h * HEAD:(h + 1) * HEAD], trig[0], trig[1])
            publish(chunk + 1, first, 4)

        for u in range(n_wide - 1):
            @pl.when(i == (u + 1) * n_k + (3 if u else -3))
            def _():
                forward(u)
        return carry

    lax.fori_loop(0, n_wide * n_k, wide_step, 0)

    def tail_step(i, carry):
        t = i + t_tail
        k = lax.rem(i, n_k)
        chunk = lax.div(i, n_k)
        tail_copy(t).wait()
        multiply(t, k, half)
        start_tile(t + SLOTS)

        @pl.when(k == n_k - 1)
        def _():
            first = 2 + 4 * n_wide + 2 * chunk
            for h in range(2):
                heads[s, first + h] = rope(acc[:, h * HEAD:(h + 1) * HEAD], trig[0], trig[1])
            publish(chunk + n_wide + 1, first, 2)

        @pl.when(i == 5)
        def _():
            forward(n_wide - 1)
        return carry

    lax.fori_loop(0, 2 * n_k, tail_step, 0)
    forward(n_wide)
    forward(n_wide + 1)
    forward(n_wide + 2)
    f_peer = lax.rem(d_peer + 2, 4)
    outs = [pltpu.make_async_copy(heads.at[g], out_hbm.at[g], out_sem.at[i]) for i, g in enumerate((s, x_peer, d_peer, f_peer))]
    outs[0].start()
    outs[1].start()
    for u, unit in enumerate(units):
        copy_of('d', d_peer, u, *unit).wait_recv()
    outs[2].start()
    for u, unit in enumerate(units):
        copy_of('f', f_peer, u, *unit).wait_recv()
    outs[3].start()
    for u, unit in enumerate(units):
        copy_of('x', s, u, *unit).wait_send()
        copy_of('d', s, u, *unit).wait_send()
        copy_of('f', x_peer, u, *unit).wait_send()
    for cp in outs:
        cp.wait()


def project(hidden, lengths, norm_gain, w_q, w_k, w_v, inv_freq):
    batch, dim = hidden.shape
    sp = 4
    n_head = w_q.shape[1] // sp // HEAD
    n_unit = n_head * HEAD // WIDE + 2
    vmem = pl.BlockSpec(memory_space=pltpu.VMEM)
    hbm = pl.BlockSpec(memory_space=pl.ANY)
    dma = pltpu.SemaphoreType.DMA
    return pl.pallas_call(
        qkv_kernel,
        out_shape=jax.ShapeDtypeStruct((sp, 2 + n_head, batch, HEAD), jnp.float32),
        in_specs=[pl.BlockSpec(memory_space=pltpu.SMEM), hbm, vmem, vmem, hbm, hbm, hbm],
        out_specs=hbm,
        scratch_shapes=[
            pltpu.VMEM((batch, dim), jnp.bfloat16),
            pltpu.VMEM((batch, dim), jnp.bfloat16),
            pltpu.VMEM((dim // HEAD, HEAD), jnp.float32),
            pltpu.VMEM((2, batch, HEAD), jnp.float32),
            pltpu.VMEM((SLOTS, KT, WIDE), jnp.bfloat16),
            pltpu.VMEM((batch, WIDE), jnp.float32),
            pltpu.VMEM((sp, 2 + n_head, batch, HEAD), jnp.float32),
            dma, dma((SLOTS,)),
            dma((n_unit,)), dma((n_unit,)), dma((n_unit,)), dma((n_unit,)), dma((n_unit,)), dma((n_unit,)),
            dma((4,)),
        ],
        compiler_params=pltpu.CompilerParams(collective_id=0, has_side_effects=True, vmem_limit_bytes=60 * MIB),
        cost_estimate=pl.CostEstimate(flops=2 * batch * dim * (n_head + 2) * HEAD, bytes_accessed=2 * dim * (n_head + 2) * HEAD, transcendentals=0),
        name='qkv_exchange',
    )(lengths, hidden, norm_gain.reshape(dim // HEAD, HEAD), inv_freq.reshape(1, HEAD // 2), w_q, w_k, w_v)


def attend_kernel(len_ref, k_hbm, v_hbm, qkv_hbm, k_out, v_out, o_ref, ml_ref,
                  qkv, qkv_sem, kbuf, vbuf, slot_of, ml_rows, k_sem, v_sem, ko_sem, vo_sem):
    batch, rows, _ = k_hbm.shape
    n_kv = 4
    slots = rows // n_kv
    n_chunk = batch // SEQS
    n_unit = qkv.shape[0] // (n_kv * batch)
    group = n_unit - 2
    n_head = n_kv * group
    start = lax.axis_index('sp') * slots

    def in_copies(i):
        r = lax.rem(i, RING)
        seqs = pl.ds(i * SEQS, SEQS)
        return (pltpu.make_async_copy(k_hbm.at[seqs], kbuf.at[r], k_sem.at[r]),
                pltpu.make_async_copy(v_hbm.at[seqs], vbuf.at[r], v_sem.at[r]))

    def out_copies(i):
        r = lax.rem(i, RING)
        seqs = pl.ds(i * SEQS, SEQS)
        return (pltpu.make_async_copy(kbuf.at[r], k_out.at[seqs], ko_sem.at[r]),
                pltpu.make_async_copy(vbuf.at[r], v_out.at[seqs], vo_sem.at[r]))

    qkv_copy = pltpu.make_async_copy(qkv_hbm, qkv, qkv_sem)
    for i in range(AHEAD):
        for cp in in_copies(i):
            cp.start()
    qkv_copy.start()

    row = lax.broadcasted_iota(jnp.int32, (n_head, rows), 0)
    col = lax.broadcasted_iota(jnp.int32, (n_head, rows), 1)
    slot_of[...] = jnp.where(lax.rem(col, n_kv) == lax.div(row, group), lax.div(col, n_kv), 2 ** 30)
    win_row = lax.broadcasted_iota(jnp.int32, (16, HEAD), 0)
    lane = lax.broadcasted_iota(jnp.int32, (n_head, HEAD), 1)

    qkv_copy.wait()

    def new_rows(offset, b):
        pairs = [qkv[pl.ds((2 * offset + i) * n_unit * batch + b, 2, stride=batch), :] for i in range(2)]
        return jnp.concatenate(pairs * 4, axis=0).astype(jnp.bfloat16)

    def chunk_step(i, carry):
        r = lax.rem(i, RING)

        @pl.when(i + AHEAD < n_chunk)
        def _():
            @pl.when(i + AHEAD >= RING)
            def _():
                for cp in out_copies(i + AHEAD - RING):
                    cp.wait()
            for cp in in_copies(i + AHEAD):
                cp.start()

        for cp in in_copies(i):
            cp.wait()
        for j in range(SEQS):
            b = i * SEQS + j
            pos = len_ref[b] - start
            held = jnp.clip(pos, 0, slots - 1)
            window = pl.ds(pl.multiple_of(lax.div(held, 4) * 16, 16), 16)
            pick = lax.div(win_row, n_kv) == jnp.where(held == pos, lax.rem(held, 4), -1)
            kbuf[r, j, window, :] = jnp.where(pick, new_rows(0, b), kbuf[r, j, window, :])
            vbuf[r, j, window, :] = jnp.where(pick, new_rows(1, b), vbuf[r, j, window, :])
        for cp in out_copies(i):
            cp.start()
        def scores_of(j):
            b = i * SEQS + j
            q = jnp.concatenate([qkv[pl.ds((g * n_unit + 2) * batch + b, group, stride=batch), :] for g in range(n_kv)], axis=0)
            return lax.dot_general(q.astype(jnp.bfloat16), kbuf[r, j], (((1,), (1,)), ((), ())), preferred_element_type=jnp.float32)

        def softmax_of(j, scores):
            valid = slot_of[...] <= len_ref[i * SEQS + j] - start
            scores = jnp.where(valid, scores, MASKED)
            top = jnp.max(scores, axis=1, keepdims=True)
            weights = jnp.where(valid, jnp.exp((scores - top) * SCALE), 0.0)
            return weights.astype(jnp.bfloat16), top, jnp.sum(weights, axis=1, keepdims=True)

        def finish(j, weights, top, total):
            b = i * SEQS + j
            o_ref[pl.ds(b, n_head, stride=batch), :] = jnp.dot(weights, vbuf[r, j], preferred_element_type=jnp.float32)
            ml_rows[pl.ds(b, n_head, stride=batch), :] = jnp.where(lane < n_head, top * SCALE, total)

        sc = [scores_of(j) for j in range(SEQS)]
        sm = [softmax_of(j, sc[j]) for j in range(SEQS)]
        for j in range(SEQS):
            finish(j, *sm[j])
        return carry

    lax.fori_loop(0, n_chunk, chunk_step, 0)
    out_lane = lax.broadcasted_iota(jnp.int32, (batch, HEAD), 1)

    def gather_step(h, acc):
        mine = lax.rem(out_lane, n_head) == h
        return jnp.where(mine, ml_rows[pl.ds(pl.multiple_of(h * batch, 8), batch), :], acc)

    ml_ref[...] = lax.fori_loop(0, n_head, gather_step, jnp.zeros((batch, HEAD), jnp.float32))

    def drain(i, carry):
        for cp in out_copies(i):
            cp.wait()
        return carry

    lax.fori_loop(n_chunk - RING, n_chunk, drain, 0)


def attend(qkv, lengths, k_cache, v_cache):
    batch, slots, n_kv, head = k_cache.shape
    rows = slots * n_kv
    n_head = n_kv * (qkv.shape[1] - 2)
    flat = (batch, rows, head)
    smem = pl.BlockSpec(memory_space=pltpu.SMEM)
    vmem = pl.BlockSpec(memory_space=pltpu.VMEM)
    hbm = pl.BlockSpec(memory_space=pl.ANY)
    dma = pltpu.SemaphoreType.DMA((RING,))
    k_new, v_new, out, ml = pl.pallas_call(
        attend_kernel,
        out_shape=(jax.ShapeDtypeStruct(flat, jnp.bfloat16), jax.ShapeDtypeStruct(flat, jnp.bfloat16),
                   jax.ShapeDtypeStruct((n_head * batch, head), jnp.float32), jax.ShapeDtypeStruct((batch, head), jnp.float32)),
        in_specs=[smem, hbm, hbm, hbm],
        out_specs=(hbm, hbm, vmem, vmem),
        scratch_shapes=[
            pltpu.VMEM((qkv.shape[0] * qkv.shape[1] * batch, head), jnp.float32), pltpu.SemaphoreType.DMA,
            pltpu.VMEM((RING, SEQS, rows, head), jnp.bfloat16),
            pltpu.VMEM((RING, SEQS, rows, head), jnp.bfloat16),
            pltpu.VMEM((n_head, rows), jnp.int32),
            pltpu.VMEM((n_head * batch, head), jnp.float32),
            dma, dma, dma, dma,
        ],
        compiler_params=pltpu.CompilerParams(vmem_limit_bytes=50 * MIB),
        cost_estimate=pl.CostEstimate(flops=4 * batch * n_head * rows * head, bytes_accessed=8 * batch * rows * head, transcendentals=0),
        name='attend_local',
    )(lengths, k_cache.reshape(flat), v_cache.reshape(flat), qkv.reshape(-1, head))
    return k_new.reshape(k_cache.shape), v_new.reshape(v_cache.shape), out, ml


def combine_kernel(own, ml_ref, hid_hbm, wo, ybf,
                   other, ml_in, ml_chip, gates, mine, x_out, x_in, d_in, obf, hid, wbuf,
                   part, part_in, fin_x, fin_d, fin_f,
                   hid_sem, w_sem, ml_send, ml_recv, o_send, o_recv, x_send, x_recv, d_send, d_recv,
                   p_send, p_recv, fx_send, fx_recv, fd_send, fd_recv, ff_send, ff_recv):
    n_head, batch, _ = own.shape
    rows = batch // 2
    half = n_head // 2
    n_piece = half // PIECE
    n_k = wo.shape[0] // OUT_K
    cols = wo.shape[1] // 2
    n_col = cols // OUT_W
    n_tile = n_col * n_k
    tp = lax.axis_index('tp')
    s = lax.axis_index('sp')
    x = lax.div(s, 2)
    c = lax.rem(s, 2)
    x_peer = lax.rem(s + 2, 4)
    d_peer = s + 1 - 2 * c
    my_rows = pl.ds(pl.multiple_of(x * rows, 16), rows)
    peer_rows = pl.ds(pl.multiple_of((1 - x) * rows, 16), rows)

    def remote(src, dst, send_sem, recv_sem, peer):
        device = {'sp': peer} if peer is not None else {'tp': 1 - tp}
        return pltpu.make_async_remote_copy(src, dst, send_sem, recv_sem, device_id=device, device_id_type=MESH_ID)

    def w_copy(t):
        lanes = pl.ds(pl.multiple_of(c * cols + lax.div(t, n_k) * OUT_W, OUT_W), OUT_W)
        depth = pl.ds(pl.multiple_of(lax.rem(t, n_k) * OUT_K, OUT_K), OUT_K)
        slot = lax.rem(t, OUT_SLOTS)
        return pltpu.make_async_copy(wo.at[depth, lanes], wbuf.at[slot], w_sem.at[slot])

    hid_copy = pltpu.make_async_copy(hid_hbm.at[my_rows, pl.ds(pl.multiple_of(c * cols, cols), cols)], hid, hid_sem)
    hid_copy.start()
    for t in range(OUT_SLOTS):
        w_copy(t).start(priority=1)

    barrier = pltpu.get_barrier_semaphore()
    for device in ({'sp': x_peer}, {'sp': d_peer}, {'tp': 1 - tp}):
        pl.semaphore_signal(barrier, inc=1, device_id=device, device_id_type=MESH_ID)
    pl.semaphore_wait(barrier, 3)

    ml_partner = remote(ml_ref, ml_in.at[0], ml_send.at[0], ml_recv.at[0], d_peer)
    ml_partner.start()

    def o_copy(p):
        return remote(own.at[pl.ds((1 - c) * half + p * PIECE, PIECE)], other.at[pl.ds(p * PIECE, PIECE)], o_send.at[p], o_recv.at[p], d_peer)

    for p in range(n_piece):
        o_copy(p).start()

    lane = lax.broadcasted_iota(jnp.int32, (batch, HEAD), 1)

    def merge_stats(first, second):
        top = jnp.maximum(first, second)
        factors = [jnp.exp(jnp.where(lane < n_head, m - top, 0.0)) for m in (first, second)]
        total = functools.reduce(jnp.add, [f * pltpu.roll(m, n_head, 1) for f, m in zip(factors, (first, second))])
        return top, factors, total

    def local_heads(per_head):
        return jnp.where(c == 0, per_head, pltpu.roll(per_head, HEAD - half, 1))

    ml_partner.wait()
    top, factors, total = merge_stats(ml_ref[...], ml_in[0])
    ml_chip[...] = jnp.where(lane < n_head, top, pltpu.roll(total, n_head, 1))
    for i in range(2):
        gates[i] = local_heads(factors[i])
    ml_x = remote(ml_chip, ml_in.at[1], ml_send.at[1], ml_recv.at[1], x_peer)

    def x_copy(p):
        part_of = pl.ds(p * PIECE, PIECE)
        return remote(x_out.at[part_of], x_in.at[part_of], x_send.at[p], x_recv.at[p], x_peer)

    def weigh(p, which):
        mine_gate = gates[0, which, :]
        other_gate = gates[1, which, :]
        out = []
        for h in range(PIECE):
            i = p * PIECE + h
            out.append(mine_gate[:, h:h + 1] * own[c * half + i, which, :] + other_gate[:, h:h + 1] * other[i, which, :])
        return out

    def mix_step(p, carry):
        o_copy(p).wait_recv()
        for h, val in enumerate(weigh(p, peer_rows)):
            x_out[p * PIECE + h] = val
        x_copy(p).start()

        @pl.when(p == 0)
        def _():
            ml_x.start()

        for h, val in enumerate(weigh(p, my_rows)):
            mine[p * PIECE + h] = val
        gates[0] = pltpu.roll(gates[0], HEAD - PIECE, 1)
        gates[1] = pltpu.roll(gates[1], HEAD - PIECE, 1)
        return carry

    lax.fori_loop(0, n_piece, mix_step, 0)
    ml_x.wait()
    top, factors, total = merge_stats(ml_chip[...], ml_in[1])
    for i in range(2):
        gates[i] = local_heads(factors[i] / total)

    def d_copy(p):
        part_of = pl.ds(p * PIECE, PIECE)
        return remote(mine.at[part_of], d_in.at[part_of], d_send.at[p], d_recv.at[p], d_peer)

    def head_lanes(h):
        return pl.ds(pl.multiple_of(h * HEAD, HEAD), HEAD)

    def merge_step(p, carry):
        x_copy(p).wait_recv()
        mine_gate = gates[0, my_rows, :]
        in_gate = gates[1, my_rows, :]
        for h in range(PIECE):
            i = p * PIECE + h
            val = (mine_gate[:, h:h + 1] * mine[i] + in_gate[:, h:h + 1] * x_in[i]).astype(jnp.bfloat16)
            obf[:, head_lanes(c * half + i)] = val
            mine[i] = val.astype(jnp.float32)
        d_copy(p).start()
        gates[0] = pltpu.roll(gates[0], HEAD - PIECE, 1)
        gates[1] = pltpu.roll(gates[1], HEAD - PIECE, 1)
        return carry

    lax.fori_loop(0, n_piece, merge_step, 0)

    def spread_step(p, carry):
        d_copy(p).wait_recv()
        for h in range(PIECE):
            i = p * PIECE + h
            obf[:, head_lanes((1 - c) * half + i)] = d_in[i].astype(jnp.bfloat16)
        return carry

    lax.fori_loop(0, n_piece, spread_step, 0)
    hid_copy.wait()

    def p_copy(j):
        return remote(part.at[j], part_in.at[j], p_send.at[j], p_recv.at[j], None)

    def fx_copy(j):
        return remote(part.at[j], fin_x.at[j], fx_send.at[j], fx_recv.at[j], x_peer)

    def fd_copy(j):
        return remote(part.at[j], fin_d.at[j], fd_send.at[j], fd_recv.at[j], d_peer)

    def ff_copy(j):
        return remote(fin_x.at[j], fin_f.at[j], ff_send.at[j], ff_recv.at[j], d_peer)

    def lanes_of(j, core):
        return pl.ds(pl.multiple_of(core * cols + j * OUT_W, OUT_W), OUT_W)

    def finish(j):
        p_copy(j).wait_recv()
        lane = pl.ds(pl.multiple_of(j * OUT_W, OUT_W), OUT_W)
        val = (hid[:, lane].astype(jnp.float32) + (part[j] + part_in[j])).astype(jnp.bfloat16)
        ybf[my_rows, lanes_of(j, c)] = val
        p_copy(j).wait_send()
        part[j] = val.astype(jnp.float32)
        fx_copy(j).start()
        fd_copy(j).start()

    def pass_on(j):
        fx_copy(j).wait_recv()
        ff_copy(j).start()
        ybf[peer_rows, lanes_of(j, c)] = fin_x[j].astype(jnp.bfloat16)
        fd_copy(j).wait_recv()
        ybf[my_rows, lanes_of(j, 1 - c)] = fin_d[j].astype(jnp.bfloat16)

    def deliver(j):
        ff_copy(j).wait_recv()
        ybf[peer_rows, lanes_of(j, 1 - c)] = fin_f[j].astype(jnp.bfloat16)

    lags = (4, 8, 10)

    def col_step(j, carry):
        @pl.when(j < n_col)
        def _():
            acc = None
            for k in range(n_k):
                t = j * n_k + k
                w_copy(t).wait()
                term = jnp.dot(obf[:, k * OUT_K:(k + 1) * OUT_K], wbuf[lax.rem(t, OUT_SLOTS)], preferred_element_type=jnp.float32)
                acc = term if acc is None else acc + term

                @pl.when(t + OUT_SLOTS < n_tile)
                def _():
                    w_copy(t + OUT_SLOTS).start(priority=1)
            part[j] = acc
            p_copy(j).start()

        for lag, stage in zip(lags, (finish, pass_on, deliver)):
            @pl.when((j >= lag) & (j - lag < n_col))
            def _():
                stage(j - lag)
        return carry

    lax.fori_loop(0, n_col + lags[-1], col_step, 0)

    for p in range(n_piece):
        o_copy(p).wait_send()
        x_copy(p).wait_send()
        d_copy(p).wait_send()

    def drain(j, carry):
        fx_copy(j).wait_send()
        fd_copy(j).wait_send()
        ff_copy(j).wait_send()
        return carry

    lax.fori_loop(0, n_col, drain, 0)


def combine(out, ml, hidden, w_o):
    batch, dim = hidden.shape
    n_head = out.shape[0] // batch
    rows = batch // 2
    half = n_head // 2
    n_piece = half // PIECE
    n_col = dim // 2 // OUT_W
    vmem = pl.BlockSpec(memory_space=pltpu.VMEM)
    hbm = pl.BlockSpec(memory_space=pl.ANY)
    dma = pltpu.SemaphoreType.DMA
    f32 = jnp.float32
    quad = pltpu.VMEM((half, rows, HEAD), f32)
    tiles = pltpu.VMEM((n_col, rows, OUT_W), f32)
    return pl.pallas_call(
        combine_kernel,
        out_shape=jax.ShapeDtypeStruct((batch, dim), jnp.bfloat16),
        in_specs=[vmem, vmem, hbm, hbm],
        out_specs=vmem,
        scratch_shapes=[
            pltpu.VMEM((half, batch, HEAD), f32),
            pltpu.VMEM((2, batch, HEAD), f32), pltpu.VMEM((batch, HEAD), f32), pltpu.VMEM((2, batch, HEAD), f32),
            quad, quad, quad, quad,
            pltpu.VMEM((rows, n_head * HEAD), jnp.bfloat16), pltpu.VMEM((rows, dim // 2), jnp.bfloat16),
            pltpu.VMEM((OUT_SLOTS, OUT_K, OUT_W), jnp.bfloat16),
            tiles, tiles, tiles, tiles, tiles,
            dma, dma((OUT_SLOTS,)), dma((2,)), dma((2,)),
            dma((n_piece,)), dma((n_piece,)), dma((n_piece,)), dma((n_piece,)), dma((n_piece,)), dma((n_piece,)),
            dma((n_col,)), dma((n_col,)), dma((n_col,)), dma((n_col,)), dma((n_col,)), dma((n_col,)), dma((n_col,)), dma((n_col,)),
        ],
        compiler_params=pltpu.CompilerParams(collective_id=1, has_side_effects=True, vmem_limit_bytes=46 * MIB),
        cost_estimate=pl.CostEstimate(flops=batch * dim * n_head * HEAD, bytes_accessed=dim * n_head * HEAD, transcendentals=0),
        name='combine_project',
    )(out.reshape(n_head, batch, HEAD), ml, hidden, w_o)


def device_step(hidden, lengths, k_cache, v_cache, norm_gain, w_q, w_k, w_v, w_o, inv_freq):
    qkv = project(hidden, lengths, norm_gain, w_q, w_k, w_v, inv_freq)
    k_new, v_new, out, ml = attend(qkv, lengths, k_cache, v_cache)
    return combine(out, ml, hidden, w_o), k_new, v_new


def solution(mesh):
    cache_spec = P('dp', 'sp', 'tp', None)
    in_specs = (P('dp', None), P('dp'), cache_spec, cache_spec, P(None), P(None, 'tp'), P(None, 'tp'), P(None, 'tp'), P('tp', None), P(None))
    out_specs = (P('dp', None), cache_spec, cache_spec)
    return jax.shard_map(device_step, mesh=mesh, in_specs=in_specs, out_specs=out_specs, check_vma=False)
```
